128 devices in a mesh: slab: 32 (over y, x, core), orb: 4 (over z).
Axes of the slice: x: 4, y: 4, z: 4, core: 2. Of those that a mesh axis runs over, the one named last changes fastest.
Arguments:
- orbitals: float32 [256, 64, 4096], P('orb', 'slab'), may hold values from -6 to 6
- pair_list: int32 [128, 2], P(('slab', 'orb')), may hold values from 0 to 255, as said below
- box_start: int32 [128, 3], P(('slab', 'orb')), may hold values from 0 to 63
Outputs:
- exchange_action: float32 [256, 64, 4096], P('orb', 'slab')
The draws below stay inside these ranges and needn't reach their ends.
Inputs may be any that keep to these rules, and one draw needn't show every extreme that they name: `pair_list`: the two orbitals of a row differ.
All inputs are finite; a program needn't handle non-finite values.
Results may differ from the reference program's by a relative error of at most 0.0003.
Values sent between devices are 32-bit elements; how exact they have to be, the bound alone decides.
A program may use at most 128 MiB of HBM per device.

```python
import jax
import jax.numpy as jnp
from jax import lax

NX = 64
NY = 64
NZ = 64
ITERS = 16
NORB = 256
NPAIRS = 128


def draw_pair_list(key, part):
    orb_key, offset_key = jax.random.split(jax.random.fold_in(key, 17))
    first_orb = jax.random.randint(orb_key, (NPAIRS,), 0, NORB)
    offset = jax.random.randint(offset_key, (NPAIRS,), 1, NORB)
    return jnp.stack([first_orb, (first_orb + offset) % NORB], axis=1).astype(jnp.int32)


def with_ends(entries, rng, low, high):
    dims = entries.shape
    index_at = [jax.random.randint(jax.random.fold_in(rng, axis), (), 0, dims[axis]) for axis in range(len(dims))]
    entries = entries.at[tuple(index_at)].set(low)
    longest = dims.index(max(dims))
    index_at[longest] = (index_at[longest] + 1) % dims[longest]
    return entries.at[tuple(index_at)].set(high)


def level_of(key, extent, cuts, least, top_value):
    factor_of, own = 1.0, jax.random.fold_in(key, 6)
    for axis_at, parts in cuts:
        steps = jnp.exp(jax.random.uniform(jax.random.fold_in(own, axis_at), (parts,), jnp.float32, least / len(cuts), top_value / len(cuts)))
        factor_of = factor_of * jnp.repeat(steps, extent[axis_at] // parts).reshape([-1 if axis == axis_at else 1 for axis in range(len(extent))])
    return factor_of


def gaussian(own_key, shape, spread, limit, shards=(), held_as=jnp.bfloat16):
    level = level_of(own_key, shape, shards, -0.22, 0.18) if shards else 1.0
    entries = jax.random.normal(own_key, shape, jnp.float32) * spread * level
    return jnp.minimum(jnp.maximum(entries, -limit), limit).astype(held_as)


def setup_inputs(seed: int = 0) -> dict:
    splits = jax.random.split(jax.random.key(seed), 4)
    orbitals = gaussian(splits[0], (NORB, NX, NY * NZ), 1.0, 6.0, ((0, 4), (1, 32)), jnp.float32)
    pair_list = draw_pair_list(jax.random.fold_in(splits[3], 71), 0)
    box_start = with_ends(jax.random.randint(splits[2], (NPAIRS, 3), 0, NX), jax.random.fold_in(splits[2], 1), 0, NX - 1).astype(jnp.int32)
    return dict(orbitals=orbitals, pair_list=pair_list, box_start=box_start)


screening = 0.02
center_eig = 6.0 + screening
half_width = 6.0
sigma_one = center_eig / half_width


def operate(field):
    grid = field.reshape(NX, NY, NZ)
    beside = jnp.roll(grid, 1, 0) + jnp.roll(grid, -1, 0)
    beside = beside + jnp.roll(grid, 1, 1) + jnp.roll(grid, -1, 1)
    beside = beside + jnp.roll(grid, 1, 2) + jnp.roll(grid, -1, 2)
    return (center_eig * grid - beside).reshape(NX, NY * NZ)


def solve_screened(density):
    def sweep(step_index, state_now):
        solution, residue, update, ratio = state_now
        solution = solution + update
        residue = residue - operate(update)
        ratio_next = 1.0 / (2.0 * sigma_one - ratio)
        update = ratio_next * ratio * update + (2.0 * ratio_next / half_width) * residue
        return (solution, residue, update, ratio_next)

    start_state = (jnp.zeros_like(density), density, density / center_eig,
                   jnp.asarray(1.0 / sigma_one, jnp.float32))
    return lax.fori_loop(0, ITERS, sweep, start_state)[0]


def box_of(corner):
    x_index = jnp.arange(NX, dtype=jnp.int32)
    cell_index = jnp.arange(NY * NZ, dtype=jnp.int32)
    y_index = cell_index // NZ
    z_index = cell_index % NZ
    inside_x = ((x_index - corner[0]) % NX) < NX // 2
    inside_y = ((y_index - corner[1]) % NY) < NY // 2
    inside_z = ((z_index - corner[2]) % NZ) < NZ // 2
    return (inside_x[:, None] & (inside_y & inside_z)[None, :]).astype(jnp.float32)


def reference(orbitals, pair_list, box_start):
    def one_pair(action, inputs):
        pair_row, corner = inputs
        first_orb = pair_row[0]
        second_orb = pair_row[1]
        mask = box_of(corner)
        left = orbitals[first_orb] * mask
        right = orbitals[second_orb] * mask
        potential = solve_screened(left * right)
        action = action.at[first_orb].add(-potential * right)
        action = action.at[second_orb].add(-potential * left)
        return action, None

    action, unused = lax.scan(one_pair, jnp.zeros_like(orbitals), (pair_list, box_start))
    return action
```

```python
import functools

import jax
import jax.numpy as jnp
import numpy as np
from jax import lax
from jax.experimental import pallas as pl
from jax.experimental.pallas import tpu as pltpu
from jax.sharding import PartitionSpec as P

ITERS = 16
SCREENING = 0.02
CENTER_EIG = 6.0 + SCREENING
HALF_WIDTH = 6.0

MESH = pl.DeviceIdType.MESH
VMEM = pl.BlockSpec(memory_space=pltpu.VMEM)
SMEM = pl.BlockSpec(memory_space=pltpu.SMEM)
F32 = jnp.float32
I32 = jnp.int32
META = 8


def chebyshev_weights():
    cheb = np.polynomial.chebyshev
    theta, delta = CENTER_EIG, HALF_WIDTH
    sigma = theta / delta
    potential, residue, update = np.zeros(1), np.ones(1), np.ones(1) / theta
    ratio = 1.0 / sigma
    for _ in range(ITERS):
        potential = cheb.chebadd(potential, update)
        applied = cheb.chebsub(theta * update, 6.0 * cheb.chebmulx(update))
        residue = cheb.chebsub(residue, applied)
        ratio_next = 1.0 / (2.0 * sigma - ratio)
        update = cheb.chebadd(ratio_next * ratio * update, 2.0 * ratio_next / delta * residue)
        ratio = ratio_next
    return [float(c) for c in potential[:ITERS]]


WEIGHTS = chebyshev_weights()


def greet(n_slab, n_orb):
    s, o = lax.axis_index("slab"), lax.axis_index("orb")
    barrier = pltpu.get_barrier_semaphore()
    for d in range(1, n_orb):
        pl.semaphore_signal(barrier, 1, device_id={"orb": lax.rem(o + d, n_orb)}, device_id_type=MESH)

    def signal(d, _):
        pl.semaphore_signal(barrier, 1, device_id={"slab": lax.rem(s + d, n_slab)}, device_id_type=MESH)
        return 0

    lax.fori_loop(1, n_slab, signal, 0)
    pl.semaphore_wait(barrier, n_orb - 1 + n_slab - 1)


def remote(src, dst, send, recv, device):
    return pltpu.make_async_remote_copy(
        src_ref=src, dst_ref=dst, send_sem=send, recv_sem=recv, device_id=device, device_id_type=MESH
    )


def share_kernel(n_slab, n_orb, row_ref, out_ref, own_sem, send_o, recv_o, send_s, recv_s):
    s, o = lax.axis_index("slab"), lax.axis_index("orb")
    own = pltpu.make_async_copy(row_ref, out_ref.at[s, o], own_sem)
    own.start()
    greet(n_slab, n_orb)
    copies = [
        remote(row_ref, out_ref.at[s, o], send_o.at[d - 1], recv_o.at[d - 1], {"orb": lax.rem(o + d, n_orb)})
        for d in range(1, n_orb)
    ]
    for copy in copies:
        copy.start()
    own.wait()
    for copy in copies:
        copy.wait()

    def to(d):
        return remote(
            out_ref.at[s], out_ref.at[s], send_s.at[d - 1], recv_s.at[d - 1], {"slab": lax.rem(s + d, n_slab)}
        )

    def start(d, _):
        to(d).start()
        return 0

    def wait(d, _):
        to(d).wait()
        return 0

    lax.fori_loop(1, n_slab, start, 0)
    lax.fori_loop(1, n_slab, wait, 0)


def lanes_and_rows():
    lane = lax.broadcasted_iota(I32, (8, 128), 1)
    row = lax.broadcasted_iota(I32, (8, 128), 0)
    return lane, row


def inside_y(j, by, lane, row):
    y = 8 * j + 2 * (row >> 1) + (lane >> 6)
    return ((y - by) & 63) < 32


def pack_kernel(n_pairs, n_orb, orb_dev, meta_ref, orb_ref, out_ref):
    o = lax.axis_index("orb")
    lane, row = lanes_and_rows()
    zz = lane & 63

    def one(p, _):
        i, j = meta_ref[META * p], meta_ref[META * p + 1]
        by, bz = meta_ref[META * p + 3], meta_ref[META * p + 4]
        hold_i, hold_j = lax.div(i, orb_dev) == o, lax.div(j, orb_dev) == o
        li, lj = lax.rem(i, orb_dev), lax.rem(j, orb_dev)
        whole = []
        for k in range(8):
            a = jnp.where(hold_i, orb_ref[li, 8 * k : 8 * k + 8, :], 1.0)
            b = jnp.where(hold_j, orb_ref[lj, 8 * k : 8 * k + 8, :], 1.0)
            whole.append(a * b)
        folded = []
        for k in range(4):
            v = jnp.where(inside_y(k, by, lane, row), whole[k], whole[k + 4])
            b = bz if k < 2 else (bz + 32) & 63
            v = jnp.where(
                zz + b < 64, pltpu.roll(v, (128 - b) & 127, 1), pltpu.roll(v, (64 - b) & 127, 1)
            )
            folded.append(v)
        for k in range(2):
            out_ref[lax.rem(p, n_orb), lax.div(p, n_orb), 8 * k : 8 * k + 8, :] = jnp.where(
                zz < 32, folded[k], folded[k + 2]
            )
        return 0

    lax.fori_loop(0, n_pairs, one, 0)


def gather_kernel(
    n_slab, n_orb, orb_dev, meta_ref, packed_ref, held_ref, box_ref,
    density, own_sem, send_o, recv_o, send_s, recv_s,
):
    s, o = lax.axis_index("slab"), lax.axis_index("orb")
    own = pltpu.make_async_copy(packed_ref.at[o], held_ref.at[o], own_sem)
    own.start()
    greet(n_slab, n_orb)
    copies = []
    for d in range(1, n_orb):
        to = lax.rem(o + d, n_orb)
        copies.append(remote(packed_ref.at[to], held_ref.at[o], send_o.at[d - 1], recv_o.at[d - 1], {"orb": to}))
    for copy in copies:
        copy.start()
    own.wait()
    for copy in copies:
        copy.wait()

    def form(q, _):
        p = q * n_orb + o
        oi, oj = lax.div(meta_ref[META * p], orb_dev), lax.div(meta_ref[META * p + 1], orb_dev)
        left = held_ref[oi, q]
        right = held_ref[oj, q]
        density[q] = jnp.where(oi == oj, left, left * right)
        return 0

    lax.fori_loop(0, n_slab, form, 0)
    mine = pltpu.make_async_copy(density.at[s], box_ref.at[s], own_sem)
    mine.start()

    def to(d):
        slab = lax.rem(s + d, n_slab)
        return remote(density.at[slab], box_ref.at[s], send_s.at[d - 1], recv_s.at[d - 1], {"slab": slab})

    def start(d, _):
        to(d).start()
        return 0

    def wait(d, _):
        to(d).wait()
        return 0

    lax.fori_loop(1, n_slab, start, 0)
    mine.wait()
    lax.fori_loop(1, n_slab, wait, 0)


def solve_kernel(start_ref, weight_ref, box_ref, out_ref, rows_a, rows_b, source, ping, pong):
    bx, by, bz = start_ref[0, 0], start_ref[0, 1], start_ref[0, 2]
    by32 = by & 31
    lane, row = lanes_and_rows()
    zz = lane & 63
    in_z = (zz >= 16) & (zz < 48)

    def place(xm, _):
        x0, x1 = (bx + xm - 8) & 63, (bx + xm + 16) & 63
        v0 = box_ref[x0 >> 1, pl.ds(x0 & 1, 8, 2), :]
        v1 = box_ref[x1 >> 1, pl.ds(x1 & 1, 8, 2), :]
        v0 = jnp.where(xm >= 8, v0, 0.0)
        v1 = jnp.where(xm < 16, v1, 0.0)
        for h in range(2):
            for q in range(2):
                a = pltpu.roll(v0, (16 - 64 * h - 32 * q) % 128, 1)
                b = pltpu.roll(v1, (80 - 64 * h - 32 * q) % 128, 1)
                v = jnp.where(in_z, jnp.where(lane < 64, a, b), 0.0)
                for dup in range(4):
                    rows_a[xm, pl.ds(32 * dup + 16 * q + h, 8, 2), :] = v
        for k in range(6):
            u = 6 * row + k - 8
            v = rows_a[xm, pl.ds(by32 + 24 + k, 8, 6), :]
            source[xm, k] = jnp.where((u >= 0) & (u < 32), v, 0.0)
        return 0

    lax.fori_loop(0, 24, place, 0)

    def close(ref):
        for k in range(6):
            ref[0, k] = pltpu.roll(ref[24, k], 64, 1)
            ref[25, k] = pltpu.roll(ref[1, k], 64, 1)

    def neighbours(ref, x):
        at = [ref[x, k] for k in range(6)]
        sums = []
        for k in range(6):
            below = at[k - 1] if k > 0 else pltpu.roll(at[5], 1, 0)
            above = at[k + 1] if k < 5 else pltpu.roll(at[0], 7, 0)
            sums.append(
                (ref[x - 1, k] + ref[x + 1, k])
                + (below + above)
                + (pltpu.roll(at[k], 1, 1) + pltpu.roll(at[k], 127, 1))
            )
        return sums

    first = weight_ref[ITERS - 1]
    for xm in range(24):
        for k in range(6):
            ping[xm + 1, k] = first * source[xm, k]
            pong[xm + 1, k] = jnp.zeros((8, 128), F32)
    close(ping)

    def step(now, older, index):
        weight = weight_ref[index]
        for xm in range(24):
            sums = neighbours(now, xm + 1)
            for k in range(6):
                older[xm + 1, k] = weight * source[xm, k] + (sums[k] * (1.0 / 3.0) - older[xm + 1, k])
        close(older)

    def two(n, _):
        step(ping, pong, ITERS - 2 - 2 * n)
        step(pong, ping, ITERS - 3 - 2 * n)
        return 0

    lax.fori_loop(0, (ITERS - 2) // 2, two, 0)
    weight = weight_ref[0]
    for xm in range(24):
        sums = neighbours(ping, xm + 1)
        for k in range(6):
            rows_b[xm, pl.ds(k, 8, 6), :] = weight * source[xm, k] + (
                sums[k] * (1.0 / 6.0) - pong[xm + 1, k]
            )

    def dup_rows(xm, _):
        for m in range(4):
            v = rows_b[xm, 8 + 8 * m : 16 + 8 * m, :]
            rows_a[xm, 8 * m : 8 * m + 8, :] = v
            rows_a[xm, 32 + 8 * m : 40 + 8 * m, :] = v
        return 0

    lax.fori_loop(0, 24, dup_rows, 0)

    def give(ux, _):
        x = (bx + ux) & 31
        half = (ux >= 16).astype(I32)
        xm = ux + 8 - 24 * half
        pieces = []
        for h in range(2):
            for q in range(2):
                v = rows_a[xm, pl.ds(32 - by32 + 16 * q + h, 8, 2), :]
                pieces.append(pltpu.roll(v, (64 * h + 32 * q - 16 + 128 - 64 * half) & 127, 1))
        v = jnp.where(
            lane < 64,
            jnp.where(zz < 32, pieces[0], pieces[1]),
            jnp.where(zz < 32, pieces[2], pieces[3]),
        )
        out_ref[x >> 1, pl.ds(x & 1, 8, 2), :] = v
        return 0

    lax.fori_loop(0, 32, give, 0)


def scatter_kernel(
    n_slab, n_orb, orb_dev, meta_ref, potential_ref, held_ref, out_ref,
    mine, terms, own_sem, send_o, recv_o, send_s, recv_s,
):
    s, o = lax.axis_index("slab"), lax.axis_index("orb")
    half = n_slab // 2
    own = pltpu.make_async_copy(potential_ref.at[lax.rem(s, half)], mine.at[s], own_sem)
    own.start()
    greet(n_slab, n_orb)

    def to(d):
        slab = lax.rem(s + d, n_slab)
        return remote(
            potential_ref.at[lax.rem(slab, half)], mine.at[s], send_s.at[d - 1], recv_s.at[d - 1], {"slab": slab}
        )

    def start(d, _):
        to(d).start()
        return 0

    def wait(d, _):
        to(d).wait()
        return 0

    lax.fori_loop(1, n_slab, start, 0)
    own.wait()
    lax.fori_loop(1, n_slab, wait, 0)

    def form(q, _):
        p = q * n_orb + o
        oi, oj = lax.div(meta_ref[META * p], orb_dev), lax.div(meta_ref[META * p + 1], orb_dev)
        value = mine[q]
        left = held_ref[oi, q]
        right = held_ref[oj, q]
        for dest in range(n_orb):
            factor = jnp.where(oi == oj, 1.0, jnp.where(oi == dest, -right, -left))
            terms[dest, q] = value * factor
        return 0

    lax.fori_loop(0, n_slab, form, 0)
    keep = pltpu.make_async_copy(terms.at[o], out_ref.at[o], own_sem)
    keep.start()
    copies = []
    for d in range(1, n_orb):
        dest = lax.rem(o + d, n_orb)
        copies.append(remote(terms.at[dest], out_ref.at[o], send_o.at[d - 1], recv_o.at[d - 1], {"orb": dest}))
    for copy in copies:
        copy.start()
    keep.wait()
    for copy in copies:
        copy.wait()


def add_kernel(n_pairs, n_orb, orb_dev, meta_ref, terms_ref, orb_ref, out_ref):
    s, o = lax.axis_index("slab"), lax.axis_index("orb")
    lane, row = lanes_and_rows()
    z = lane & 63
    x = 2 * s + (row & 1)

    def clear(n, _):
        out_ref[n] = jnp.zeros(out_ref.shape[1:], F32)
        return 0

    lax.fori_loop(0, orb_dev, clear, 0)

    def one(p, _):
        i, j = meta_ref[META * p], meta_ref[META * p + 1]
        bx, by, bz = meta_ref[META * p + 2], meta_ref[META * p + 3], meta_ref[META * p + 4]
        hold_i, hold_j = lax.div(i, orb_dev) == o, lax.div(j, orb_dev) == o
        li, lj = lax.rem(i, orb_dev), lax.rem(j, orb_dev)

        def unfolded():
            in_xz = (((x - bx) & 63) < 32) & (((z - bz) & 63) < 32)
            wide = []
            for k in range(4):
                v = terms_ref[lax.rem(p, n_orb), lax.div(p, n_orb), 8 * (k % 2) : 8 * (k % 2) + 8, :]
                b = bz if k < 2 else (bz + 32) & 63
                v = jnp.where(z >= b, pltpu.roll(v, b, 1), pltpu.roll(v, (b + 64) & 127, 1))
                wide.append(jnp.where(in_xz, v, 0.0))
            keep = [inside_y(k, by, lane, row) for k in range(4)]
            return [jnp.where(keep[k], wide[k], 0.0) for k in range(4)] + [
                jnp.where(keep[k], 0.0, wide[k]) for k in range(4)
            ]

        both = hold_i & hold_j

        @pl.when(both)
        def _():
            values = unfolded()
            for k in range(8):
                rows = slice(8 * k, 8 * k + 8)
                out_ref[li, rows, :] = out_ref[li, rows, :] - values[k] * orb_ref[lj, rows, :]
                out_ref[lj, rows, :] = out_ref[lj, rows, :] - values[k] * orb_ref[li, rows, :]

        @pl.when((hold_i | hold_j) & jnp.logical_not(both))
        def _():
            at = jnp.where(hold_i, li, lj)
            values = unfolded()
            for k in range(8):
                rows = slice(8 * k, 8 * k + 8)
                out_ref[at, rows, :] = out_ref[at, rows, :] + values[k]

        return 0

    lax.fori_loop(0, n_pairs, one, 0)


def peer_sems(n_slab, n_orb):
    return [
        pltpu.SemaphoreType.DMA,
        pltpu.SemaphoreType.DMA((n_orb - 1,)),
        pltpu.SemaphoreType.DMA((n_orb - 1,)),
        pltpu.SemaphoreType.DMA((n_slab - 1,)),
        pltpu.SemaphoreType.DMA((n_slab - 1,)),
    ]


def remote_params(identity):
    return pltpu.CompilerParams(collective_id=identity, has_side_effects=True, vmem_limit_bytes=40 << 20)


def body(orbitals, pair_list, box_start):
    n_slab, n_orb = lax.axis_size("slab"), lax.axis_size("orb")
    orb_dev, planes, cells = orbitals.shape
    n_pairs = n_slab * n_orb
    slot = (16, 128)
    rows = orbitals.reshape(orb_dev, planes, cells // 128, 128).transpose(0, 2, 1, 3)
    rows = rows.reshape(orb_dev, planes * cells // 128, 128)
    own = jnp.pad(jnp.concatenate([pair_list, box_start], axis=1), ((0, 0), (0, 123)))
    meta = pl.pallas_call(
        functools.partial(share_kernel, n_slab, n_orb),
        out_shape=jax.ShapeDtypeStruct((n_slab, n_orb, 1, 128), I32),
        in_specs=[VMEM],
        out_specs=VMEM,
        scratch_shapes=peer_sems(n_slab, n_orb),
        compiler_params=remote_params(0),
        name="share",
    )(own)
    meta = meta.reshape(n_pairs, 128)[:, :META].reshape(-1)
    packed = pl.pallas_call(
        functools.partial(pack_kernel, n_pairs, n_orb, orb_dev),
        out_shape=jax.ShapeDtypeStruct((n_orb, n_slab) + slot, F32),
        in_specs=[SMEM, VMEM],
        out_specs=VMEM,
        name="pack",
    )(meta, rows)
    held, box = pl.pallas_call(
        functools.partial(gather_kernel, n_slab, n_orb, orb_dev),
        out_shape=[
            jax.ShapeDtypeStruct((n_orb, n_slab) + slot, F32),
            jax.ShapeDtypeStruct((n_slab,) + slot, F32),
        ],
        in_specs=[SMEM, VMEM],
        out_specs=[VMEM, VMEM],
        scratch_shapes=[pltpu.VMEM((n_slab,) + slot, F32)] + peer_sems(n_slab, n_orb),
        compiler_params=remote_params(1),
        name="gather",
    )(meta, packed)
    weights = jnp.asarray(np.asarray(WEIGHTS, np.float32))
    potential = pl.pallas_call(
        solve_kernel,
        out_shape=jax.ShapeDtypeStruct((n_slab // 2,) + slot, F32),
        in_specs=[SMEM, SMEM, VMEM],
        out_specs=VMEM,
        scratch_shapes=[
            pltpu.VMEM((24, 128, 128), F32),
            pltpu.VMEM((24, 48, 128), F32),
            pltpu.VMEM((24, 6, 8, 128), F32),
            pltpu.VMEM((26, 6, 8, 128), F32),
            pltpu.VMEM((26, 6, 8, 128), F32),
        ],
        name="solve",
    )(box_start, weights, box)
    terms = pl.pallas_call(
        functools.partial(scatter_kernel, n_slab, n_orb, orb_dev),
        out_shape=jax.ShapeDtypeStruct((n_orb, n_slab) + slot, F32),
        in_specs=[SMEM, VMEM, VMEM],
        out_specs=VMEM,
        scratch_shapes=[
            pltpu.VMEM((n_slab,) + slot, F32),
            pltpu.VMEM((n_orb, n_slab) + slot, F32),
        ]
        + peer_sems(n_slab, n_orb),
        compiler_params=remote_params(2),
        name="scatter",
    )(meta, potential, held)
    action = pl.pallas_call(
        functools.partial(add_kernel, n_pairs, n_orb, orb_dev),
        out_shape=jax.ShapeDtypeStruct(rows.shape, F32),
        in_specs=[SMEM, VMEM, VMEM],
        out_specs=VMEM,
        name="add",
    )(meta, terms, rows)
    action = action.reshape(orb_dev, cells // 128, planes, 128).transpose(0, 2, 1, 3)
    return action.reshape(orb_dev, planes, cells)


def solution(mesh):
    return jax.shard_map(
        body,
        mesh=mesh,
        in_specs=(P("orb", "slab", None), P(("slab", "orb"), None), P(("slab", "orb"), None)),
        out_specs=P("orb", "slab", None),
        check_vma=False,
    )
```

```python
import functools

import jax
import jax.numpy as jnp
import numpy as np
from jax import lax
from jax.experimental import pallas as pl
from jax.experimental.pallas import tpu as pltpu
from jax.sharding import PartitionSpec as P

ITERS = 16
SCREENING = 0.02
CENTER_EIG = 6.0 + SCREENING
HALF_WIDTH = 6.0

MESH = pl.DeviceIdType.MESH
VMEM = pl.BlockSpec(memory_space=pltpu.VMEM)
SMEM = pl.BlockSpec(memory_space=pltpu.SMEM)
F32 = jnp.float32
I32 = jnp.int32
META = 8
CHUNKS = 4
UNROLL = 4


def chebyshev_weights():
    cheb = np.polynomial.chebyshev
    theta, delta = CENTER_EIG, HALF_WIDTH
    sigma = theta / delta
    potential, residue, update = np.zeros(1), np.ones(1), np.ones(1) / theta
    ratio = 1.0 / sigma
    for _ in range(ITERS):
        potential = cheb.chebadd(potential, update)
        applied = cheb.chebsub(theta * update, 6.0 * cheb.chebmulx(update))
        residue = cheb.chebsub(residue, applied)
        ratio_next = 1.0 / (2.0 * sigma - ratio)
        update = cheb.chebadd(ratio_next * ratio * update, 2.0 * ratio_next / delta * residue)
        ratio = ratio_next
    return [float(c) for c in potential[:ITERS]]


WEIGHTS = chebyshev_weights()


def greet(n_slab, n_orb):
    s, o = lax.axis_index("slab"), lax.axis_index("orb")
    barrier = pltpu.get_barrier_semaphore()
    for d in range(1, n_orb):
        pl.semaphore_signal(barrier, 1, device_id={"orb": lax.rem(o + d, n_orb)}, device_id_type=MESH)

    def signal(d, _):
        pl.semaphore_signal(barrier, 1, device_id={"slab": lax.rem(s + d, n_slab)}, device_id_type=MESH)
        return 0

    lax.fori_loop(1, n_slab, signal, 0)
    pl.semaphore_wait(barrier, n_orb - 1 + n_slab - 1)


def remote(src, dst, send, recv, device):
    return pltpu.make_async_remote_copy(
        src_ref=src, dst_ref=dst, send_sem=send, recv_sem=recv, device_id=device, device_id_type=MESH
    )


def lanes_and_rows():
    lane = lax.broadcasted_iota(I32, (8, 128), 1)
    row = lax.broadcasted_iota(I32, (8, 128), 0)
    return lane, row


def inside_y(j, by, lane, row):
    y = 8 * j + 2 * (row >> 1) + (lane >> 6)
    return ((y - by) & 63) < 32


def pair_of(meta_ref, p, n_orb):
    slab, base = lax.div(p, n_orb), META * lax.rem(p, n_orb)
    return [meta_ref[slab, 0, base + k] for k in range(5)]


def loop(low, high, step):
    def run(n, carry):
        step(n)
        return carry

    lax.fori_loop(low, high, run, 0)


def unrolled(low, high, step):
    def run(n, carry):
        step(n)
        return carry

    lax.fori_loop(low, high, run, 0, unroll=UNROLL)


def share(n_slab, n_orb, pair_ref, start_ref, row, trio, joined, meta_v, meta_s, own_sem, send_o, recv_o, send_s, recv_s):
    s, o = lax.axis_index("slab"), lax.axis_index("orb")
    lane = lax.broadcasted_iota(I32, (1, 128), 1) - META * o
    values = [pair_ref[0, 0], pair_ref[0, 1], start_ref[0, 0], start_ref[0, 1], start_ref[0, 2]]
    line = jnp.zeros((1, 128), I32)
    for k, value in enumerate(values):
        line = jnp.where(lane == k, value, line)
    row[...] = line
    trio[o] = line
    greet(n_slab, n_orb)
    copies = [
        remote(row, trio.at[o], send_o.at[d - 1], recv_o.at[d - 1], {"orb": lax.rem(o + d, n_orb)})
        for d in range(1, n_orb)
    ]
    for copy in copies:
        copy.start()
    for copy in copies:
        copy.wait()
    total = trio[0]
    for k in range(1, n_orb):
        total = total + trio[k]
    joined[...] = total
    meta_v[s] = total

    def to(d):
        return remote(joined, meta_v.at[s], send_s.at[d - 1], recv_s.at[d - 1], {"slab": lax.rem(s + d, n_slab)})

    loop(1, n_slab, lambda d: to(d).start())
    loop(1, n_slab, lambda d: to(d).wait())
    local = pltpu.make_async_copy(meta_v, meta_s, own_sem)
    local.start()
    local.wait()


def pack_one(n_orb, orb_dev, meta, orb, packed, dest, q):
    o = lax.axis_index("orb")
    lane, row = lanes_and_rows()
    zz = lane & 63
    i, j, _, by, bz = pair_of(meta, q * n_orb + dest, n_orb)
    hold_i, hold_j = lax.div(i, orb_dev) == o, lax.div(j, orb_dev) == o
    li, lj = lax.rem(i, orb_dev), lax.rem(j, orb_dev)
    whole = []
    for k in range(8):
        a = jnp.where(hold_i, orb[li, 8 * k : 8 * k + 8, :], 1.0)
        b = jnp.where(hold_j, orb[lj, 8 * k : 8 * k + 8, :], 1.0)
        whole.append(a * b)
    folded = []
    for k in range(4):
        v = jnp.where(inside_y(k, by, lane, row), whole[k], whole[k + 4])
        b = bz if k < 2 else (bz + 32) & 63
        folded.append(
            jnp.where(zz + b < 64, pltpu.roll(v, (128 - b) & 127, 1), pltpu.roll(v, (64 - b) & 127, 1))
        )
    for k in range(2):
        packed[dest, q, 8 * k : 8 * k + 8, :] = jnp.where(zz < 32, folded[k], folded[k + 2])


class Ring:
    def __init__(self, n_slab, n_orb, source, target, relay, near_sem, first_sem, last_sem):
        self.o, self.n_orb = lax.axis_index("orb"), n_orb
        self.size, self.source, self.target, self.relay = n_slab // CHUNKS, source, target, relay
        self.near_sem, self.first_sem, self.last_sem = near_sem, first_sem, last_sem

    def plane(self, d):
        return lax.rem(self.o + d, self.n_orb)

    def rows(self, c):
        return pl.ds(c * self.size, self.size)

    def near(self, d, c):
        n = (0 if d == 1 else 1) * CHUNKS + c
        return remote(
            self.source.at[self.plane(d), self.rows(c)], self.target.at[self.o, self.rows(c)],
            self.near_sem.at[0, n], self.near_sem.at[1, n], {"orb": self.plane(d)},
        )

    def first(self, c):
        way = 1 if c < CHUNKS // 2 else self.n_orb - 1
        return remote(
            self.source.at[self.plane(2), self.rows(c)], self.relay.at[c],
            self.first_sem.at[0, c], self.first_sem.at[1, c], {"orb": self.plane(way)},
        )

    def last(self, c):
        way = 1 if c < CHUNKS // 2 else self.n_orb - 1
        return remote(
            self.relay.at[c], self.target.at[self.plane(self.n_orb - way), self.rows(c)],
            self.last_sem.at[0, c], self.last_sem.at[1, c], {"orb": self.plane(way)},
        )

    def pass_on(self, c):
        self.first(c).wait_recv()
        self.last(c).start()

    def arrived(self, c):
        self.near(1, c).wait_recv()
        self.near(self.n_orb - 1, c).wait_recv()
        self.last(c).wait_recv()

    def drain(self):
        for c in range(CHUNKS):
            self.near(1, c).wait_send()
            self.near(self.n_orb - 1, c).wait_send()
            self.first(c).wait_send()
            self.last(c).wait_send()


def solve(start_ref, weight_ref, box, out, rows_a, rows_b, source, ping, pong):
    bx, by = start_ref[0, 0], start_ref[0, 1]
    by32 = by & 31
    lane, row = lanes_and_rows()
    zz = lane & 63
    in_z = (zz >= 16) & (zz < 48)

    def place(xm):
        x0, x1 = (bx + xm - 8) & 63, (bx + xm + 16) & 63
        v0 = jnp.where(xm >= 8, box[x0 >> 1, pl.ds(x0 & 1, 8, 2), :], 0.0)
        v1 = jnp.where(xm < 16, box[x1 >> 1, pl.ds(x1 & 1, 8, 2), :], 0.0)
        for h in range(2):
            for q in range(2):
                a = pltpu.roll(v0, (16 - 64 * h - 32 * q) % 128, 1)
                b = pltpu.roll(v1, (80 - 64 * h - 32 * q) % 128, 1)
                v = jnp.where(in_z, jnp.where(lane < 64, a, b), 0.0)
                for dup in range(4):
                    rows_a[xm, pl.ds(32 * dup + 16 * q + h, 8, 2), :] = v

    unrolled(0, 24, place)

    first = weight_ref[ITERS - 1]

    def fill(xm):
        for k in range(6):
            u = 6 * row + k - 8
            v = rows_a[xm, pl.ds(by32 + 24 + k, 8, 6), :]
            v = jnp.where((u >= 0) & (u < 32), v, 0.0)
            source[xm, k] = v
            ping[xm + 1, k] = first * v
            pong[xm + 1, k] = jnp.zeros((8, 128), F32)

    unrolled(0, 24, fill)

    def close(ref):
        for k in range(6):
            ref[0, k] = pltpu.roll(ref[24, k], 64, 1)
            ref[25, k] = pltpu.roll(ref[1, k], 64, 1)

    def neighbours(ref, x):
        at = [ref[x, k] for k in range(6)]
        sums = []
        for k in range(6):
            below = at[k - 1] if k > 0 else pltpu.roll(at[5], 1, 0)
            above = at[k + 1] if k < 5 else pltpu.roll(at[0], 7, 0)
            sums.append(
                (ref[x - 1, k] + ref[x + 1, k])
                + (below + above)
                + (pltpu.roll(at[k], 1, 1) + pltpu.roll(at[k], 127, 1))
            )
        return sums

    close(ping)

    def step(now, older, index):
        weight = weight_ref[index]
        for xm in range(24):
            sums = neighbours(now, xm + 1)
            for k in range(6):
                older[xm + 1, k] = weight * source[xm, k] + (sums[k] * (1.0 / 3.0) - older[xm + 1, k])
        close(older)

    def two(n):
        step(ping, pong, ITERS - 2 - 2 * n)
        step(pong, ping, ITERS - 3 - 2 * n)

    loop(0, (ITERS - 2) // 2, two)
    weight = weight_ref[0]
    for xm in range(24):
        sums = neighbours(ping, xm + 1)
        for k in range(6):
            rows_b[xm, pl.ds(k, 8, 6), :] = weight * source[xm, k] + (sums[k] * (1.0 / 6.0) - pong[xm + 1, k])

    def twice(xm):
        for m in range(4):
            v = rows_b[xm, 8 + 8 * m : 16 + 8 * m, :]
            rows_a[xm, 8 * m : 8 * m + 8, :] = v
            rows_a[xm, 32 + 8 * m : 40 + 8 * m, :] = v

    unrolled(0, 24, twice)

    def give(x2):
        for plane in range(2):
            ux = (2 * x2 + plane - bx) & 31
            half = (ux >= 16).astype(I32)
            xm = ux + 8 - 24 * half
            pieces = []
            for h in range(2):
                for q in range(2):
                    v = rows_a[xm, pl.ds(32 - by32 + 16 * q + h, 8, 2), :]
                    pieces.append(pltpu.roll(v, (64 * h + 32 * q - 16 + 128 - 64 * half) & 127, 1))
            v = jnp.where(
                lane < 64,
                jnp.where(zz < 32, pieces[0], pieces[1]),
                jnp.where(zz < 32, pieces[2], pieces[3]),
            )
            out[x2, pl.ds(plane, 8, 2), :] = v

    unrolled(0, 16, give)


def main_kernel(
    n_slab, n_orb, orb_dev, pair_ref, start_ref, weight_ref, orb_hbm, terms, meta_v,
    row, trio, joined, meta_s, orb, packed, held, relay, density, box, rows_a, rows_b, source, ping, pong,
    potential, mine, outgoing, relay_back,
    own_sem, load_sem, send_o, recv_o, send_m, recv_m, near_a, first_a, last_a, near_b, first_b, last_b,
    send_d, recv_d, send_p, recv_p,
):
    s, o = lax.axis_index("slab"), lax.axis_index("orb")
    half = n_slab // 2
    load = pltpu.make_async_copy(orb_hbm, orb, load_sem)
    load.start()
    share(n_slab, n_orb, pair_ref, start_ref, row, trio, joined, meta_v, meta_s, own_sem, send_o, recv_o, send_m, recv_m)
    load.wait()

    ring = Ring(n_slab, n_orb, packed, held, relay, near_a, first_a, last_a)
    size = ring.size

    def pack(d, c):
        dest = ring.plane(d)
        into = held if d == 0 else packed
        unrolled(c * size, (c + 1) * size, lambda q: pack_one(n_orb, orb_dev, meta_s, orb, into, dest, q))

    for c in (0, 2, 1, 3):
        pack(2, c)
        ring.first(c).start()
    for c in range(CHUNKS):
        for d in (1, n_orb - 1):
            pack(d, c)
            ring.near(d, c).start()
    for c in (0, 2, 1, 3):
        ring.pass_on(c)
    for c in range(CHUNKS):
        pack(0, c)

    def holders(q):
        i, j, _, _, _ = pair_of(meta_s, q * n_orb + o, n_orb)
        return lax.div(i, orb_dev), lax.div(j, orb_dev)

    def to_owner(q):
        return remote(density.at[q], box.at[s], send_d.at[q], recv_d.at[s], {"slab": q})

    def from_slab(q):
        return remote(density.at[q], box.at[q], send_d.at[q], recv_d.at[q], {"slab": q})

    def pick(q, plane):
        value = held[0, q]
        for k in range(1, n_orb):
            value = jnp.where(plane == k, held[k, q], value)
        return value

    def form(q):
        oi, oj = holders(q)
        left, right = pick(q, oi), pick(q, oj)
        density[q] = jnp.where(oi == oj, left, left * right)

    def send_density(q):
        @pl.when(q != s)
        def _():
            to_owner(q).start()

    for c in range(CHUNKS):
        ring.arrived(c)
        unrolled(c * size, (c + 1) * size, form)
        loop(c * size, (c + 1) * size, send_density)
    box[s] = density[s]
    loop(1, n_slab, lambda d: from_slab(lax.rem(s + d, n_slab)).wait_recv())

    solve(start_ref, weight_ref, box, potential, rows_a, rows_b, source, ping, pong)

    def to_slab(q):
        return remote(potential.at[lax.rem(q, half)], mine.at[s], send_p.at[q], recv_p.at[s], {"slab": q})

    def from_owner(q):
        return remote(potential.at[lax.rem(q, half)], mine.at[q], send_p.at[q], recv_p.at[q], {"slab": q})

    loop(1, n_slab, lambda d: to_slab(lax.rem(s + d, n_slab)).start())
    mine[s] = potential[lax.rem(s, half)]
    back = Ring(n_slab, n_orb, outgoing, terms, relay_back, near_b, first_b, last_b)

    def wait_mine(q):
        @pl.when(q != s)
        def _():
            from_owner(q).wait_recv()

    def term(d, q):
        dest = back.plane(d)
        oi, oj = holders(q)
        left, right = held[oi, q], held[oj, q]
        factor = jnp.where(oi == oj, 1.0, jnp.where(oi == dest, -right, -left))
        into = terms if d == 0 else outgoing
        into[dest, q] = mine[q] * factor

    for c in (0, 2, 1, 3):
        loop(c * size, (c + 1) * size, wait_mine)
        unrolled(c * size, (c + 1) * size, lambda q: term(2, q))
        back.first(c).start()
    for c in range(CHUNKS):
        for d in (1, n_orb - 1):
            unrolled(c * size, (c + 1) * size, lambda q: term(d, q))
            back.near(d, c).start()
    for c in (0, 2, 1, 3):
        back.pass_on(c)
    unrolled(0, n_slab, lambda q: term(0, q))
    for c in range(CHUNKS):
        back.arrived(c)
    ring.drain()
    back.drain()

    def drain(d):
        q = lax.rem(s + d, n_slab)
        to_owner(q).wait_send()
        to_slab(q).wait_send()

    loop(1, n_slab, drain)


def add_kernel(n_pairs, n_orb, orb_dev, meta_ref, terms_ref, orb_hbm, out_ref, orb_ref, load_sem):
    s, o = lax.axis_index("slab"), lax.axis_index("orb")
    load = pltpu.make_async_copy(orb_hbm, orb_ref, load_sem)
    load.start()
    lane, row = lanes_and_rows()
    z = lane & 63
    x = 2 * s + (row & 1)

    def clear(n):
        out_ref[n] = jnp.zeros(out_ref.shape[1:], F32)

    loop(0, orb_dev, clear)
    load.wait()

    def one(p):
        i, j, bx, by, bz = pair_of(meta_ref, p, n_orb)
        hold_i, hold_j = lax.div(i, orb_dev) == o, lax.div(j, orb_dev) == o
        li, lj = lax.rem(i, orb_dev), lax.rem(j, orb_dev)

        def unfolded():
            in_xz = (((x - bx) & 63) < 32) & (((z - bz) & 63) < 32)
            wide = []
            for k in range(4):
                v = terms_ref[lax.rem(p, n_orb), lax.div(p, n_orb), 8 * (k % 2) : 8 * (k % 2) + 8, :]
                b = bz if k < 2 else (bz + 32) & 63
                v = jnp.where(z >= b, pltpu.roll(v, b, 1), pltpu.roll(v, (b + 64) & 127, 1))
                wide.append(jnp.where(in_xz, v, 0.0))
            keep = [inside_y(k, by, lane, row) for k in range(4)]
            return [jnp.where(keep[k], wide[k], 0.0) for k in range(4)] + [
                jnp.where(keep[k], 0.0, wide[k]) for k in range(4)
            ]

        both = hold_i & hold_j

        @pl.when(both)
        def _():
            values = unfolded()
            for k in range(8):
                rows = slice(8 * k, 8 * k + 8)
                out_ref[li, rows, :] = out_ref[li, rows, :] - values[k] * orb_ref[lj, rows, :]
                out_ref[lj, rows, :] = out_ref[lj, rows, :] - values[k] * orb_ref[li, rows, :]

        @pl.when((hold_i | hold_j) & jnp.logical_not(both))
        def _():
            at = jnp.where(hold_i, li, lj)
            values = unfolded()
            for k in range(8):
                rows = slice(8 * k, 8 * k + 8)
                out_ref[at, rows, :] = out_ref[at, rows, :] + values[k]

    loop(0, n_pairs, one)


def body(orbitals, pair_list, box_start):
    n_slab, n_orb = lax.axis_size("slab"), lax.axis_size("orb")
    orb_dev, planes, cells = orbitals.shape
    n_pairs = n_slab * n_orb
    slot = (16, 128)
    slots = (n_orb, n_slab) + slot
    rows = orbitals.reshape(orb_dev, planes, cells // 128, 128).transpose(0, 2, 1, 3)
    rows = rows.reshape(orb_dev, planes * cells // 128, 128)
    weights = jnp.asarray(np.asarray(WEIGHTS, np.float32))
    relay = pltpu.VMEM((CHUNKS, n_slab // CHUNKS) + slot, F32)
    dma = pltpu.SemaphoreType.DMA
    ring_sems = [dma((2, 2 * CHUNKS)), dma((2, CHUNKS)), dma((2, CHUNKS))]
    terms, meta = pl.pallas_call(
        functools.partial(main_kernel, n_slab, n_orb, orb_dev),
        out_shape=[jax.ShapeDtypeStruct(slots, F32), jax.ShapeDtypeStruct((n_slab, 1, 128), I32)],
        in_specs=[SMEM, SMEM, SMEM, pl.BlockSpec(memory_space=pl.ANY)],
        out_specs=[VMEM, VMEM],
        scratch_shapes=[
            pltpu.VMEM((1, 128), I32),
            pltpu.VMEM((n_orb, 1, 128), I32),
            pltpu.VMEM((1, 128), I32),
            pltpu.SMEM((n_slab, 1, 128), I32),
            pltpu.VMEM(rows.shape, F32),
            pltpu.VMEM(slots, F32),
            pltpu.VMEM(slots, F32),
            relay,
            pltpu.VMEM((n_slab,) + slot, F32),
            pltpu.VMEM((n_slab,) + slot, F32),
            pltpu.VMEM((24, 128, 128), F32),
            pltpu.VMEM((24, 48, 128), F32),
            pltpu.VMEM((24, 6, 8, 128), F32),
            pltpu.VMEM((26, 6, 8, 128), F32),
            pltpu.VMEM((26, 6, 8, 128), F32),
            pltpu.VMEM((n_slab // 2,) + slot, F32),
            pltpu.VMEM((n_slab,) + slot, F32),
            pltpu.VMEM(slots, F32),
            relay,
            dma,
            dma,
            dma((n_orb - 1,)),
            dma((n_orb - 1,)),
            dma((n_slab - 1,)),
            dma((n_slab - 1,)),
        ]
        + ring_sems
        + ring_sems
        + [dma((n_slab,))] * 4,
        compiler_params=pltpu.CompilerParams(collective_id=0, has_side_effects=True, vmem_limit_bytes=40 << 20),
        name="exchange",
    )(pair_list, box_start, weights, rows)
    action = pl.pallas_call(
        functools.partial(add_kernel, n_pairs, n_orb, orb_dev),
        out_shape=jax.ShapeDtypeStruct(rows.shape, F32),
        in_specs=[SMEM, VMEM, pl.BlockSpec(memory_space=pl.ANY)],
        out_specs=VMEM,
        scratch_shapes=[pltpu.VMEM(rows.shape, F32), dma],
        name="add",
    )(meta, terms, rows)
    action = action.reshape(orb_dev, cells // 128, planes, 128).transpose(0, 2, 1, 3)
    return action.reshape(orb_dev, planes, cells)


def solution(mesh):
    return jax.shard_map(
        body,
        mesh=mesh,
        in_specs=(P("orb", "slab", None), P(("slab", "orb"), None), P(("slab", "orb"), None)),
        out_specs=P("orb", "slab", None),
        check_vma=False,
    )
```

```python
import functools

import jax
import jax.numpy as jnp
import numpy as np
from jax import lax
from jax.experimental import pallas as pl
from jax.experimental.pallas import tpu as pltpu
from jax.sharding import PartitionSpec as P

ITERS = 16
SCREENING = 0.02
CENTER_EIG = 6.0 + SCREENING
HALF_WIDTH = 6.0

MESH = pl.DeviceIdType.MESH
VMEM = pl.BlockSpec(memory_space=pltpu.VMEM)
SMEM = pl.BlockSpec(memory_space=pltpu.SMEM)
F32 = jnp.float32
I32 = jnp.int32
META = 8
CHUNKS = 4
EXCHANGE_VMEM = 50 << 20
UNROLL = 4


def chebyshev_weights():
    cheb = np.polynomial.chebyshev
    theta, delta = CENTER_EIG, HALF_WIDTH
    sigma = theta / delta
    potential, residue, update = np.zeros(1), np.ones(1), np.ones(1) / theta
    ratio = 1.0 / sigma
    for _ in range(ITERS):
        potential = cheb.chebadd(potential, update)
        applied = cheb.chebsub(theta * update, 6.0 * cheb.chebmulx(update))
        residue = cheb.chebsub(residue, applied)
        ratio_next = 1.0 / (2.0 * sigma - ratio)
        update = cheb.chebadd(ratio_next * ratio * update, 2.0 * ratio_next / delta * residue)
        ratio = ratio_next
    return [float(c) for c in potential[:ITERS]]


WEIGHTS = chebyshev_weights()


def greet(n_slab, n_orb):
    s, o = lax.axis_index("slab"), lax.axis_index("orb")
    barrier = pltpu.get_barrier_semaphore()
    for d in range(1, n_orb):
        pl.semaphore_signal(barrier, 1, device_id={"orb": lax.rem(o + d, n_orb)}, device_id_type=MESH)

    def signal(d, _):
        pl.semaphore_signal(barrier, 1, device_id={"slab": lax.rem(s + d, n_slab)}, device_id_type=MESH)
        return 0

    lax.fori_loop(1, n_slab, signal, 0)
    pl.semaphore_wait(barrier, n_orb - 1 + n_slab - 1)


def remote(src, dst, send, recv, device):
    return pltpu.make_async_remote_copy(
        src_ref=src, dst_ref=dst, send_sem=send, recv_sem=recv, device_id=device, device_id_type=MESH
    )


def lanes_and_rows():
    lane = lax.broadcasted_iota(I32, (8, 128), 1)
    row = lax.broadcasted_iota(I32, (8, 128), 0)
    return lane, row


def inside_y(j, by, lane, row):
    y = 8 * j + 2 * (row >> 1) + (lane >> 6)
    return ((y - by) & 63) < 32


def split(index, count):
    if count & (count - 1):
        return lax.div(index, count), lax.rem(index, count)
    return index >> (count.bit_length() - 1), index & (count - 1)


def pair_of(meta_ref, p, n_orb):
    slab, at = split(p, n_orb)
    return [meta_ref[slab, 0, META * at + k] for k in range(5)]


def loop(low, high, step):
    def run(n, carry):
        step(n)
        return carry

    lax.fori_loop(low, high, run, 0)


def unrolled(low, high, step):
    def run(n, carry):
        step(n)
        return carry

    lax.fori_loop(low, high, run, 0, unroll=UNROLL)


def share(n_slab, n_orb, own_ref, row, trio, joined, meta_v, send_o, recv_o, send_m, recv_m):
    s, o = lax.axis_index("slab"), lax.axis_index("orb")
    row[...] = jnp.zeros((1, 128), I32)
    row[:, 0:5] = own_ref[...]
    line = pltpu.roll(jnp.broadcast_to(row[...], (8, 128)), META * o, 1)[0:1, :]
    row[...] = line
    trio[o] = line
    copies = [
        remote(row, trio.at[o], send_o.at[d - 1], recv_o.at[d - 1], {"orb": lax.rem(o + d, n_orb)})
        for d in range(1, n_orb)
    ]
    for copy in copies:
        copy.start()
    for copy in copies:
        copy.wait()
    total = trio[0]
    for k in range(1, n_orb):
        total = total + trio[k]
    joined[...] = total
    meta_v[s] = total

    def to(q):
        return remote(joined, meta_v.at[s], send_m.at[q], recv_m.at[s], {"slab": q})

    def arrived(q):
        @pl.when(q != s)
        def _():
            remote(joined, meta_v.at[q], send_m.at[q], recv_m.at[q], {"slab": q}).wait_recv()

    loop(1, n_slab, lambda d: to(lax.rem(s + d, n_slab)).start())
    return arrived, lambda d: to(lax.rem(s + d, n_slab)).wait_send()


def pack_one(n_orb, orb_dev, meta, orb, packed, dest, q):
    o = lax.axis_index("orb")
    lane, row = lanes_and_rows()
    zz = lane & 63
    i, j, _, by, bz = pair_of(meta, q * n_orb + dest, n_orb)
    (oi, li), (oj, lj) = split(i, orb_dev), split(j, orb_dev)
    hold_i, hold_j = oi == o, oj == o
    whole = []
    for k in range(8):
        a = jnp.where(hold_i, orb[li, 8 * k : 8 * k + 8, :], 1.0)
        b = jnp.where(hold_j, orb[lj, 8 * k : 8 * k + 8, :], 1.0)
        whole.append(a * b)
    folded = []
    for k in range(4):
        v = jnp.where(inside_y(k, by, lane, row), whole[k], whole[k + 4])
        b = bz if k < 2 else (bz + 32) & 63
        folded.append(
            jnp.where(zz + b < 64, pltpu.roll(v, (128 - b) & 127, 1), pltpu.roll(v, (64 - b) & 127, 1))
        )
    for k in range(2):
        packed[dest, q, 8 * k : 8 * k + 8, :] = jnp.where(zz < 32, folded[k], folded[k + 2])


def weight_of(index):
    value = jnp.float32(WEIGHTS[0])
    for k in range(1, ITERS):
        value = jnp.where(index == k, jnp.float32(WEIGHTS[k]), value)
    return value


def solve(bx, by, box, out, rows_a, rows_b, source, ping, pong):
    by32 = by & 31
    lane, row = lanes_and_rows()
    zz = lane & 63
    in_z = (zz >= 16) & (zz < 48)

    def place(xm):
        x0, x1 = (bx + xm - 8) & 63, (bx + xm + 16) & 63
        v0 = jnp.where(xm >= 8, box[x0 >> 1, pl.ds(x0 & 1, 8, 2), :], 0.0)
        v1 = jnp.where(xm < 16, box[x1 >> 1, pl.ds(x1 & 1, 8, 2), :], 0.0)
        for h in range(2):
            for q in range(2):
                a = pltpu.roll(v0, (16 - 64 * h - 32 * q) % 128, 1)
                b = pltpu.roll(v1, (80 - 64 * h - 32 * q) % 128, 1)
                v = jnp.where(in_z, jnp.where(lane < 64, a, b), 0.0)
                for dup in range(4):
                    rows_a[xm, pl.ds(32 * dup + 16 * q + h, 8, 2), :] = v

    unrolled(0, 24, place)

    first = WEIGHTS[ITERS - 1]

    def fill(xm):
        for k in range(6):
            u = 6 * row + k - 8
            v = rows_a[xm, pl.ds(by32 + 24 + k, 8, 6), :]
            v = jnp.where((u >= 0) & (u < 32), v, 0.0)
            source[xm, k] = v
            ping[xm + 1, k] = first * v
            pong[xm + 1, k] = jnp.zeros((8, 128), F32)

    unrolled(0, 24, fill)

    def close(ref):
        for k in range(6):
            ref[0, k] = pltpu.roll(ref[24, k], 64, 1)
            ref[25, k] = pltpu.roll(ref[1, k], 64, 1)

    def neighbours(ref, x):
        at = [ref[x, k] for k in range(6)]
        sums = []
        for k in range(6):
            below = at[k - 1] if k > 0 else pltpu.roll(at[5], 1, 0)
            above = at[k + 1] if k < 5 else pltpu.roll(at[0], 7, 0)
            sums.append(
                (ref[x - 1, k] + ref[x + 1, k])
                + (below + above)
                + (pltpu.roll(at[k], 1, 1) + pltpu.roll(at[k], 127, 1))
            )
        return sums

    close(ping)

    def step(now, older, index):
        weight = weight_of(index)
        for xm in range(24):
            sums = neighbours(now, xm + 1)
            for k in range(6):
                older[xm + 1, k] = weight * source[xm, k] + (sums[k] * (1.0 / 3.0) - older[xm + 1, k])
        close(older)

    def two(n):
        step(ping, pong, ITERS - 2 - 2 * n)
        step(pong, ping, ITERS - 3 - 2 * n)

    loop(0, (ITERS - 2) // 2, two)
    weight = WEIGHTS[0]
    for xm in range(24):
        sums = neighbours(ping, xm + 1)
        for k in range(6):
            rows_b[xm, pl.ds(k, 8, 6), :] = weight * source[xm, k] + (sums[k] * (1.0 / 6.0) - pong[xm + 1, k])

    def twice(xm):
        for m in range(4):
            v = rows_b[xm, 8 + 8 * m : 16 + 8 * m, :]
            rows_a[xm, 8 * m : 8 * m + 8, :] = v
            rows_a[xm, 32 + 8 * m : 40 + 8 * m, :] = v

    unrolled(0, 24, twice)

    def give(x2):
        for plane in range(2):
            ux = (2 * x2 + plane - bx) & 31
            half = (ux >= 16).astype(I32)
            xm = ux + 8 - 24 * half
            pieces = []
            for h in range(2):
                for q in range(2):
                    v = rows_a[xm, pl.ds(32 - by32 + 16 * q + h, 8, 2), :]
                    pieces.append(pltpu.roll(v, (64 * h + 32 * q - 16 + 128 - 64 * half) & 127, 1))
            v = jnp.where(
                lane < 64,
                jnp.where(zz < 32, pieces[0], pieces[1]),
                jnp.where(zz < 32, pieces[2], pieces[3]),
            )
            out[x2, pl.ds(plane, 8, 2), :] = v

    unrolled(0, 16, give)


def main_kernel(
    n_slab, n_orb, orb_dev, own_ref, orb_hbm, terms, meta_hbm, orb,
    row, trio, joined, meta_v, meta_s, packed, held, relay, combined, density, box,
    rows_a, rows_b, source, ping, pong, potential, mine, to_relay, to_plain, to_far, from_dest,
    load_sem, meta_sem, send_o, recv_o, send_m, recv_m, ring_sem, back_sem, send_d, recv_d, send_p, recv_p,
):
    s, o = lax.axis_index("slab"), lax.axis_index("orb")
    half, size = n_slab // 2, n_slab // CHUNKS
    load = pltpu.make_async_copy(orb_hbm, orb, load_sem)
    load.start()
    greet(n_slab, n_orb)
    row_arrived, row_sent = share(
        n_slab, n_orb, own_ref, row, trio, joined, meta_v, send_o, recv_o, send_m, recv_m
    )

    chunks = [(lax.rem(lax.div(s, size) + k, CHUNKS), way) for k, way in ((0, 1), (2, -1), (1, 1), (3, -1))]

    def plane(d):
        return lax.rem(o + d + n_orb, n_orb)

    def rows(c):
        return pl.ds(c * size, size)

    def chunk_loop(c, step):
        unrolled(0, size, lambda n: step(c * size + n, n))

    def ring_copy(kind, sems, source, target, c, d):
        return remote(source, target, sems.at[kind, 0, c], sems.at[kind, 1, c], {"orb": plane(d)})

    def far(c, way):
        return ring_copy(0, ring_sem, packed.at[plane(2), rows(c)], relay.at[c], c, way)

    def through(c, way):
        return ring_copy(1, ring_sem, combined.at[c], held.at[o, rows(c)], c, way)

    def straight(c, way):
        return ring_copy(2, ring_sem, packed.at[plane(-way), rows(c)], held.at[o, rows(c)], c, -way)

    def pack(d, c, into):
        dest = plane(d)
        chunk_loop(c, lambda q, n: pack_one(n_orb, orb_dev, meta_s, orb, into, dest, q))

    def pass_on(c, way):
        far(c, way).wait_recv()

        def step(q, n):
            combined[c, n] = relay[c, n] * packed[plane(way), q]

        chunk_loop(c, step)
        through(c, way).start()

    for at, (c, way) in enumerate(chunks):
        loop(c * size, (c + 1) * size, row_arrived)
        local = pltpu.make_async_copy(meta_v.at[rows(c)], meta_s.at[rows(c)], meta_sem.at[0])
        local.start()
        local.wait()
        if at == 0:
            load.wait()
        pack(2, c, packed)
        far(c, way).start()
        pack(-way, c, packed)
        straight(c, way).start()
        pack(way, c, packed)
        if at > 0:
            pass_on(*chunks[at - 1])
    keep = pltpu.make_async_copy(meta_v, meta_hbm, meta_sem.at[1])
    keep.start()
    pass_on(*chunks[-1])
    for c, _ in chunks:
        pack(0, c, held)

    def to_owner(q):
        return remote(density.at[q], box.at[s], send_d.at[q], recv_d.at[s], {"slab": q})

    def from_slab(q):
        return remote(density.at[q], box.at[q], send_d.at[q], recv_d.at[q], {"slab": q})

    def send_density(q):
        @pl.when(q != s)
        def _():
            to_owner(q).start()

    for c, way in chunks:
        through(c, way).wait_recv()
        straight(c, way).wait_recv()

        def form(q, n):
            density[q] = held[o, q] * (held[plane(1), q] * held[plane(-1), q])

        chunk_loop(c, form)
        loop(c * size, (c + 1) * size, send_density)
    box[s] = density[s]
    loop(1, n_slab, lambda d: from_slab(lax.rem(s + d, n_slab)).wait_recv())

    _, _, bx, by, _ = pair_of(meta_s, s * n_orb + o, n_orb)
    solve(bx, by, box, potential, rows_a, rows_b, source, ping, pong)

    def to_slab(q):
        return remote(potential.at[lax.rem(q, half)], mine.at[s], send_p.at[q], recv_p.at[s], {"slab": q})

    def from_owner(q):
        return remote(potential.at[lax.rem(q, half)], mine.at[q], send_p.at[q], recv_p.at[q], {"slab": q})

    def send_potential(q):
        @pl.when(q != s)
        def _():
            to_slab(q).start()

    def wait_mine(q):
        @pl.when(q != s)
        def _():
            from_owner(q).wait_recv()

    for c, _ in chunks:
        loop(c * size, (c + 1) * size, send_potential)
    mine[s] = potential[lax.rem(s, half)]

    def back_relay(c, way):
        return ring_copy(0, back_sem, to_relay.at[c], from_dest.at[c], c, -way)

    def back_straight(c, way):
        return ring_copy(1, back_sem, to_plain.at[c], terms.at[o, rows(c)], c, way)

    def back_far(c, way):
        return ring_copy(2, back_sem, to_far.at[c], terms.at[plane(way), rows(c)], c, -way)

    def finish(c, way):
        back_relay(c, way).wait_recv()

        def step(q, n):
            value = from_dest[c, n]
            to_far[c, n] = value * packed[plane(way), q]
            terms[plane(way), q] = value * relay[c, n]

        chunk_loop(c, step)
        back_far(c, way).start()

    for at, (c, way) in enumerate(chunks):
        loop(c * size, (c + 1) * size, wait_mine)

        def share_out(q, n):
            own = mine[q] * held[o, q]
            to_relay[c, n] = own * held[plane(way), q]
            to_plain[c, n] = own * held[plane(-way), q]

        chunk_loop(c, share_out)
        back_relay(c, way).start()
        back_straight(c, way).start()
        if at > 0:
            finish(*chunks[at - 1])
    finish(*chunks[-1])
    for c, _ in chunks:

        def own_term(q, n):
            terms[o, q] = mine[q] * (held[plane(1), q] * held[plane(-1), q])

        chunk_loop(c, own_term)
    for c, way in chunks:
        back_straight(c, way).wait_recv()
        back_far(c, way).wait_recv()
    for c, way in chunks:
        for copy in (far, through, straight, back_relay, back_straight, back_far):
            copy(c, way).wait_send()

    def drain(d):
        q = lax.rem(s + d, n_slab)
        row_sent(d)
        to_owner(q).wait_send()
        to_slab(q).wait_send()

    loop(1, n_slab, drain)
    keep.wait()


def add_kernel(n_pairs, n_orb, orb_dev, meta_ref, terms_ref, orb_ref, out_ref):
    s, o = lax.axis_index("slab"), lax.axis_index("orb")
    lane, row = lanes_and_rows()
    z = lane & 63
    x = 2 * s + (row & 1)

    def clear(n):
        out_ref[n] = jnp.zeros(out_ref.shape[1:], F32)

    loop(0, orb_dev, clear)

    def one(p):
        i, j, bx, by, bz = pair_of(meta_ref, p, n_orb)
        (oi, li), (oj, lj) = split(i, orb_dev), split(j, orb_dev)
        hold_i, hold_j = oi == o, oj == o

        owner_slab, owner_orb = split(p, n_orb)

        def unfolded():
            in_xz = (((x - bx) & 63) < 32) & (((z - bz) & 63) < 32)
            wide = []
            for k in range(4):
                v = terms_ref[owner_orb, owner_slab, 8 * (k % 2) : 8 * (k % 2) + 8, :]
                b = bz if k < 2 else (bz + 32) & 63
                v = jnp.where(z >= b, pltpu.roll(v, b, 1), pltpu.roll(v, (b + 64) & 127, 1))
                wide.append(jnp.where(in_xz, v, 0.0))
            keep = [inside_y(k, by, lane, row) for k in range(4)]
            return [jnp.where(keep[k], wide[k], 0.0) for k in range(4)] + [
                jnp.where(keep[k], 0.0, wide[k]) for k in range(4)
            ]

        both = hold_i & hold_j

        @pl.when(both)
        def _():
            values = unfolded()
            for k in range(8):
                rows = slice(8 * k, 8 * k + 8)
                out_ref[li, rows, :] = out_ref[li, rows, :] - values[k] * orb_ref[lj, rows, :]
                out_ref[lj, rows, :] = out_ref[lj, rows, :] - values[k] * orb_ref[li, rows, :]

        @pl.when((hold_i | hold_j) & jnp.logical_not(both))
        def _():
            at = jnp.where(hold_i, li, lj)
            values = unfolded()
            for k in range(8):
                rows = slice(8 * k, 8 * k + 8)
                out_ref[at, rows, :] = out_ref[at, rows, :] - values[k]

    loop(0, n_pairs, one)


def body(orbitals, pair_list, box_start):
    n_slab, n_orb = lax.axis_size("slab"), lax.axis_size("orb")
    orb_dev, planes, cells = orbitals.shape
    n_pairs = n_slab * n_orb
    slot = (16, 128)
    slots = (n_orb, n_slab) + slot
    rows = orbitals.reshape(orb_dev, planes, cells // 128, 128).transpose(0, 2, 1, 3)
    rows = rows.reshape(orb_dev, planes * cells // 128, 128)
    dma = pltpu.SemaphoreType.DMA
    hbm = pl.BlockSpec(memory_space=pltpu.HBM)
    all_slots, chunked = pltpu.VMEM(slots, F32), pltpu.VMEM((CHUNKS, n_slab // CHUNKS) + slot, F32)
    slabs = pltpu.VMEM((n_slab,) + slot, F32)
    own = jnp.concatenate([pair_list, box_start], axis=1)
    terms, meta, orb_near = pl.pallas_call(
        functools.partial(main_kernel, n_slab, n_orb, orb_dev),
        out_shape=[
            jax.ShapeDtypeStruct(slots, F32),
            jax.ShapeDtypeStruct((n_slab, 1, 128), I32),
            jax.ShapeDtypeStruct(rows.shape, F32),
        ],
        in_specs=[VMEM, hbm],
        out_specs=[VMEM, hbm, VMEM],
        scratch_shapes=[
            pltpu.VMEM((1, 128), I32),
            pltpu.VMEM((n_orb, 1, 128), I32),
            pltpu.VMEM((1, 128), I32),
            pltpu.VMEM((n_slab, 1, 128), I32),
            pltpu.SMEM((n_slab, 1, 128), I32),
            all_slots,
            all_slots,
            chunked,
            chunked,
            slabs,
            slabs,
            pltpu.VMEM((24, 128, 128), F32),
            pltpu.VMEM((24, 48, 128), F32),
            pltpu.VMEM((24, 6, 8, 128), F32),
            pltpu.VMEM((26, 6, 8, 128), F32),
            pltpu.VMEM((26, 6, 8, 128), F32),
            pltpu.VMEM((n_slab // 2,) + slot, F32),
            slabs,
            chunked,
            chunked,
            chunked,
            chunked,
            dma,
            dma((2,)),
            dma((n_orb - 1,)),
            dma((n_orb - 1,)),
            dma((n_slab,)),
            dma((n_slab,)),
            dma((3, 2, CHUNKS)),
            dma((3, 2, CHUNKS)),
            dma((n_slab,)),
            dma((n_slab,)),
            dma((n_slab,)),
            dma((n_slab,)),
        ],
        compiler_params=pltpu.CompilerParams(collective_id=0, has_side_effects=True, vmem_limit_bytes=EXCHANGE_VMEM),
        name="exchange",
    )(own, rows)
    action = pl.pallas_call(
        functools.partial(add_kernel, n_pairs, n_orb, orb_dev),
        out_shape=jax.ShapeDtypeStruct(rows.shape, F32),
        in_specs=[SMEM, VMEM, VMEM],
        out_specs=VMEM,
        compiler_params=pltpu.CompilerParams(vmem_limit_bytes=16 << 20),
        name="add",
    )(meta, terms, orb_near)
    action = action.reshape(orb_dev, cells // 128, planes, 128).transpose(0, 2, 1, 3)
    return action.reshape(orb_dev, planes, cells)


def solution(mesh):
    return jax.shard_map(
        body,
        mesh=mesh,
        in_specs=(P("orb", "slab", None), P(("slab", "orb"), None), P(("slab", "orb"), None)),
        out_specs=P("orb", "slab", None),
        check_vma=False,
    )
```

```python
import functools

import jax
import jax.numpy as jnp
import numpy as np
from jax import lax
from jax.experimental import pallas as pl
from jax.experimental.pallas import tpu as pltpu
from jax.sharding import PartitionSpec as P

ITERS = 16
SCREENING = 0.02
CENTER_EIG = 6.0 + SCREENING
HALF_WIDTH = 6.0

MESH = pl.DeviceIdType.MESH
VMEM = pl.BlockSpec(memory_space=pltpu.VMEM)
SMEM = pl.BlockSpec(memory_space=pltpu.SMEM)
F32 = jnp.float32
I32 = jnp.int32
META = 8
CHUNKS = 4
EXCHANGE_VMEM = 50 << 20
UNROLL = 4
TOGETHER = 4


def chebyshev_weights():
    cheb = np.polynomial.chebyshev
    theta, delta = CENTER_EIG, HALF_WIDTH
    sigma = theta / delta
    potential, residue, update = np.zeros(1), np.ones(1), np.ones(1) / theta
    ratio = 1.0 / sigma
    for _ in range(ITERS):
        potential = cheb.chebadd(potential, update)
        applied = cheb.chebsub(theta * update, 6.0 * cheb.chebmulx(update))
        residue = cheb.chebsub(residue, applied)
        ratio_next = 1.0 / (2.0 * sigma - ratio)
        update = cheb.chebadd(ratio_next * ratio * update, 2.0 * ratio_next / delta * residue)
        ratio = ratio_next
    return [float(c) for c in potential[:ITERS]]


WEIGHTS = chebyshev_weights()


def greet(n_slab, n_orb):
    s, o = lax.axis_index("slab"), lax.axis_index("orb")
    barrier = pltpu.get_barrier_semaphore()
    for d in range(1, n_orb):
        pl.semaphore_signal(barrier, 1, device_id={"orb": lax.rem(o + d, n_orb)}, device_id_type=MESH)

    def signal(d, _):
        pl.semaphore_signal(barrier, 1, device_id={"slab": lax.rem(s + d, n_slab)}, device_id_type=MESH)
        return 0

    lax.fori_loop(1, n_slab, signal, 0)
    pl.semaphore_wait(barrier, n_orb - 1 + n_slab - 1)


def remote(src, dst, send, recv, device):
    return pltpu.make_async_remote_copy(
        src_ref=src, dst_ref=dst, send_sem=send, recv_sem=recv, device_id=device, device_id_type=MESH
    )


def lanes_and_rows():
    lane = lax.broadcasted_iota(I32, (8, 128), 1)
    row = lax.broadcasted_iota(I32, (8, 128), 0)
    return lane, row


def inside_y(j, by, lane, row):
    y = 8 * j + 2 * (row >> 1) + (lane >> 6)
    return ((y - by) & 63) < 32


def split(index, count):
    if count & (count - 1):
        return lax.div(index, count), lax.rem(index, count)
    return index >> (count.bit_length() - 1), index & (count - 1)


def pair_of(meta_ref, p, n_orb):
    slab, at = split(p, n_orb)
    return [meta_ref[slab, 0, META * at + k] for k in range(5)]


def loop(low, high, step):
    def run(n, carry):
        step(n)
        return carry

    lax.fori_loop(low, high, run, 0)


def unrolled(low, high, step):
    def run(n, carry):
        step(n)
        return carry

    lax.fori_loop(low, high, run, 0, unroll=UNROLL)


def share(n_slab, n_orb, own_ref, row, trio, joined, meta_v, send_o, recv_o, send_m, recv_m):
    s, o = lax.axis_index("slab"), lax.axis_index("orb")
    row[...] = jnp.zeros((1, 128), I32)
    row[:, 0:5] = own_ref[...]
    line = pltpu.roll(jnp.broadcast_to(row[...], (8, 128)), META * o, 1)[0:1, :]
    row[...] = line
    trio[o] = line
    copies = [
        remote(row, trio.at[o], send_o.at[d - 1], recv_o.at[d - 1], {"orb": lax.rem(o + d, n_orb)})
        for d in range(1, n_orb)
    ]
    for copy in copies:
        copy.start()
    for copy in copies:
        copy.wait()
    total = trio[0]
    for k in range(1, n_orb):
        total = total + trio[k]
    joined[...] = total
    meta_v[s] = total

    def to(q):
        return remote(joined, meta_v.at[s], send_m.at[q], recv_m.at[s], {"slab": q})

    def arrived(q):
        @pl.when(q != s)
        def _():
            remote(joined, meta_v.at[q], send_m.at[q], recv_m.at[q], {"slab": q}).wait_recv()

    loop(1, n_slab, lambda d: to(lax.rem(s + d, n_slab)).start())
    return arrived, lambda d: to(lax.rem(s + d, n_slab)).wait_send()


def pack_one(n_orb, orb_dev, meta, orb, packed, dest, q):
    o = lax.axis_index("orb")
    lane, row = lanes_and_rows()
    zz = lane & 63
    i, j, _, by, bz = pair_of(meta, q * n_orb + dest, n_orb)
    (oi, li), (oj, lj) = split(i, orb_dev), split(j, orb_dev)
    hold_i, hold_j = oi == o, oj == o
    whole = []
    for k in range(8):
        a = jnp.where(hold_i, orb[li, 8 * k : 8 * k + 8, :], 1.0)
        b = jnp.where(hold_j, orb[lj, 8 * k : 8 * k + 8, :], 1.0)
        whole.append(a * b)
    folded = []
    for k in range(4):
        v = jnp.where(inside_y(k, by, lane, row), whole[k], whole[k + 4])
        b = bz if k < 2 else (bz + 32) & 63
        folded.append(
            jnp.where(zz + b < 64, pltpu.roll(v, (128 - b) & 127, 1), pltpu.roll(v, (64 - b) & 127, 1))
        )
    for k in range(2):
        packed[dest, q, 8 * k : 8 * k + 8, :] = jnp.where(zz < 32, folded[k], folded[k + 2])


def weight_of(index):
    value = jnp.float32(WEIGHTS[0])
    for k in range(1, ITERS):
        value = jnp.where(index == k, jnp.float32(WEIGHTS[k]), value)
    return value


def solve(bx, by, box, out, rows_a, rows_b, source, ping, pong):
    by32 = by & 31
    lane, row = lanes_and_rows()
    zz = lane & 63
    in_z = (zz >= 16) & (zz < 48)

    def place(xm):
        x0, x1 = (bx + xm - 8) & 63, (bx + xm + 16) & 63
        v0 = jnp.where(xm >= 8, box[x0 >> 1, pl.ds(x0 & 1, 8, 2), :], 0.0)
        v1 = jnp.where(xm < 16, box[x1 >> 1, pl.ds(x1 & 1, 8, 2), :], 0.0)
        for h in range(2):
            for q in range(2):
                a = pltpu.roll(v0, (16 - 64 * h - 32 * q) % 128, 1)
                b = pltpu.roll(v1, (80 - 64 * h - 32 * q) % 128, 1)
                v = jnp.where(in_z, jnp.where(lane < 64, a, b), 0.0)
                for dup in range(4):
                    rows_a[xm, pl.ds(32 * dup + 16 * q + h, 8, 2), :] = v

    unrolled(0, 24, place)

    first = WEIGHTS[ITERS - 1]

    def fill(xm):
        for k in range(6):
            u = 6 * row + k - 8
            v = rows_a[xm, pl.ds(by32 + 24 + k, 8, 6), :]
            v = jnp.where((u >= 0) & (u < 32), v, 0.0)
            source[xm, k] = v
            ping[xm + 1, k] = first * v
            pong[xm + 1, k] = jnp.zeros((8, 128), F32)

    unrolled(0, 24, fill)

    def close(ref):
        for k in range(6):
            ref[0, k] = pltpu.roll(ref[24, k], 64, 1)
            ref[25, k] = pltpu.roll(ref[1, k], 64, 1)

    def neighbours(ref, x):
        at = [ref[x, k] for k in range(6)]
        sums = []
        for k in range(6):
            below = at[k - 1] if k > 0 else pltpu.roll(at[5], 1, 0)
            above = at[k + 1] if k < 5 else pltpu.roll(at[0], 7, 0)
            sums.append(
                (ref[x - 1, k] + ref[x + 1, k])
                + (below + above)
                + (pltpu.roll(at[k], 1, 1) + pltpu.roll(at[k], 127, 1))
            )
        return sums

    close(ping)

    def step(now, older, index):
        weight = weight_of(index)
        for xm in range(24):
            sums = neighbours(now, xm + 1)
            for k in range(6):
                older[xm + 1, k] = weight * source[xm, k] + (sums[k] * (1.0 / 3.0) - older[xm + 1, k])
        close(older)

    def two(n):
        step(ping, pong, ITERS - 2 - 2 * n)
        step(pong, ping, ITERS - 3 - 2 * n)

    loop(0, (ITERS - 2) // 2, two)
    weight = WEIGHTS[0]
    for xm in range(24):
        sums = neighbours(ping, xm + 1)
        for k in range(6):
            rows_b[xm, pl.ds(k, 8, 6), :] = weight * source[xm, k] + (sums[k] * (1.0 / 6.0) - pong[xm + 1, k])

    def twice(xm):
        for m in range(4):
            v = rows_b[xm, 8 + 8 * m : 16 + 8 * m, :]
            rows_a[xm, 8 * m : 8 * m + 8, :] = v
            rows_a[xm, 32 + 8 * m : 40 + 8 * m, :] = v

    unrolled(0, 24, twice)

    def give(x2):
        for plane in range(2):
            ux = (2 * x2 + plane - bx) & 31
            half = (ux >= 16).astype(I32)
            xm = ux + 8 - 24 * half
            pieces = []
            for h in range(2):
                for q in range(2):
                    v = rows_a[xm, pl.ds(32 - by32 + 16 * q + h, 8, 2), :]
                    pieces.append(pltpu.roll(v, (64 * h + 32 * q - 16 + 128 - 64 * half) & 127, 1))
            v = jnp.where(
                lane < 64,
                jnp.where(zz < 32, pieces[0], pieces[1]),
                jnp.where(zz < 32, pieces[2], pieces[3]),
            )
            out[x2, pl.ds(plane, 8, 2), :] = v

    unrolled(0, 16, give)


def main_kernel(
    n_slab, n_orb, orb_dev, own_ref, orb_hbm, terms, meta_hbm, orb,
    row, trio, joined, meta_v, meta_s, packed, held, relay, combined, density, box,
    rows_a, rows_b, source, ping, pong, potential, mine, to_relay, to_plain, to_far, from_dest,
    load_sem, meta_sem, send_o, recv_o, send_m, recv_m, ring_sem, back_sem, send_d, recv_d, send_p, recv_p,
):
    s, o = lax.axis_index("slab"), lax.axis_index("orb")
    half, size = n_slab // 2, n_slab // CHUNKS
    load = pltpu.make_async_copy(orb_hbm, orb, load_sem)
    load.start()
    greet(n_slab, n_orb)
    row_arrived, row_sent = share(
        n_slab, n_orb, own_ref, row, trio, joined, meta_v, send_o, recv_o, send_m, recv_m
    )

    chunks = [(lax.rem(lax.div(s, size) + k, CHUNKS), way) for k, way in ((0, 1), (2, -1), (1, 1), (3, -1))]

    def plane(d):
        return lax.rem(o + d + n_orb, n_orb)

    def rows(c):
        return pl.ds(c * size, size)

    def chunk_loop(c, step):
        unrolled(0, size, lambda n: step(c * size + n, n))

    def ring_copy(kind, sems, source, target, c, d):
        return remote(source, target, sems.at[kind, 0, c], sems.at[kind, 1, c], {"orb": plane(d)})

    def far(c, way):
        return ring_copy(0, ring_sem, packed.at[plane(2), rows(c)], relay.at[c], c, way)

    def through(c, way):
        return ring_copy(1, ring_sem, combined.at[c], held.at[o, rows(c)], c, way)

    def straight(c, way):
        return ring_copy(2, ring_sem, packed.at[plane(-way), rows(c)], held.at[o, rows(c)], c, -way)

    def pack(d, c, into):
        dest = plane(d)
        chunk_loop(c, lambda q, n: pack_one(n_orb, orb_dev, meta_s, orb, into, dest, q))

    def pass_on(c, way):
        far(c, way).wait_recv()

        def step(q, n):
            combined[c, n] = relay[c, n] * packed[plane(way), q]

        chunk_loop(c, step)
        through(c, way).start()

    for at, (c, way) in enumerate(chunks):
        loop(c * size, (c + 1) * size, row_arrived)
        local = pltpu.make_async_copy(meta_v.at[rows(c)], meta_s.at[rows(c)], meta_sem.at[0])
        local.start()
        local.wait()
        if at == 0:
            load.wait()
        pack(2, c, packed)
        far(c, way).start()
    keep = pltpu.make_async_copy(meta_v, meta_hbm, meta_sem.at[1])
    keep.start()
    for c, way in chunks:
        pack(-way, c, packed)
        straight(c, way).start()
    for c, way in chunks:
        pack(way, c, packed)
        pass_on(c, way)
    for c, _ in chunks:
        pack(0, c, held)

    def to_owner(q):
        return remote(density.at[q], box.at[s], send_d.at[q], recv_d.at[s], {"slab": q})

    def from_slab(q):
        return remote(density.at[q], box.at[q], send_d.at[q], recv_d.at[q], {"slab": q})

    def send_density(q):
        @pl.when(q != s)
        def _():
            to_owner(q).start()

    for c, way in chunks:
        through(c, way).wait_recv()
        straight(c, way).wait_recv()

        def form(q, n):
            density[q] = held[o, q] * (held[plane(1), q] * held[plane(-1), q])

        chunk_loop(c, form)
        loop(c * size, (c + 1) * size, send_density)
    box[s] = density[s]
    loop(1, n_slab, lambda d: from_slab(lax.rem(s + d, n_slab)).wait_recv())

    _, _, bx, by, _ = pair_of(meta_s, s * n_orb + o, n_orb)
    solve(bx, by, box, potential, rows_a, rows_b, source, ping, pong)

    def to_slab(q):
        return remote(potential.at[lax.rem(q, half)], mine.at[s], send_p.at[q], recv_p.at[s], {"slab": q})

    def from_owner(q):
        return remote(potential.at[lax.rem(q, half)], mine.at[q], send_p.at[q], recv_p.at[q], {"slab": q})

    def send_potential(q):
        @pl.when(q != s)
        def _():
            to_slab(q).start()

    def wait_mine(q):
        @pl.when(q != s)
        def _():
            from_owner(q).wait_recv()

    for c, _ in chunks:
        loop(c * size, (c + 1) * size, send_potential)
    mine[s] = potential[lax.rem(s, half)]

    def back_relay(c, way):
        return ring_copy(0, back_sem, to_relay.at[c], from_dest.at[c], c, -way)

    def back_straight(c, way):
        return ring_copy(1, back_sem, to_plain.at[c], terms.at[o, rows(c)], c, way)

    def back_far(c, way):
        return ring_copy(2, back_sem, to_far.at[c], terms.at[plane(way), rows(c)], c, -way)

    def finish(c, way):
        back_relay(c, way).wait_recv()

        def step(q, n):
            value = from_dest[c, n]
            to_far[c, n] = value * packed[plane(way), q]
            terms[plane(way), q] = value * relay[c, n]

        chunk_loop(c, step)
        back_far(c, way).start()

    for c, way in chunks:
        loop(c * size, (c + 1) * size, wait_mine)

        def share_out(q, n):
            own = mine[q] * held[o, q]
            to_relay[c, n] = own * held[plane(way), q]
            to_plain[c, n] = own * held[plane(-way), q]

        chunk_loop(c, share_out)
        back_relay(c, way).start()
        back_straight(c, way).start()
    for c, way in chunks:
        finish(c, way)
    for c, _ in chunks:

        def own_term(q, n):
            terms[o, q] = mine[q] * (held[plane(1), q] * held[plane(-1), q])

        chunk_loop(c, own_term)
    for c, way in chunks:
        back_straight(c, way).wait_recv()
        back_far(c, way).wait_recv()
    for c, way in chunks:
        for copy in (far, through, straight, back_relay, back_straight, back_far):
            copy(c, way).wait_send()

    def drain(d):
        q = lax.rem(s + d, n_slab)
        row_sent(d)
        to_owner(q).wait_send()
        to_slab(q).wait_send()

    loop(1, n_slab, drain)
    keep.wait()


def add_kernel(n_pairs, n_orb, orb_dev, meta_ref, terms_ref, orb_ref, out_ref, entries):
    s, o = lax.axis_index("slab"), lax.axis_index("orb")
    lane, row = lanes_and_rows()
    z = lane & 63
    x = 2 * s + (row & 1)
    clear = out_ref.shape[1] * orb_dev // n_pairs

    def collect(p, count):
        i, j = pair_of(meta_ref, p, n_orb)[:2]
        (oi, li), (oj, lj) = split(i, orb_dev), split(j, orb_dev)
        both = (oi == oj).astype(I32) * orb_dev
        entries[count] = ((both + lj) * orb_dev + li) * n_pairs + p
        count = count + (oi == o).astype(I32)
        entries[count] = ((both + li) * orb_dev + lj) * n_pairs + p
        count = count + (oj == o).astype(I32)
        at, part = split(p, n_pairs // orb_dev)
        out_ref[at, pl.ds(pl.multiple_of(part * clear, clear), clear), :] = jnp.zeros((clear, 128), F32)
        return count

    count = lax.fori_loop(0, n_pairs, collect, 0, unroll=UNROLL)
    for k in range(TOGETHER):
        entries[count + k] = 0

    def value_of(index):
        rest, p = split(entries[index], n_pairs)
        rest, at = split(rest, orb_dev)
        both, other = split(rest, orb_dev)
        _, _, bx, by, bz = pair_of(meta_ref, p, n_orb)
        owner_slab, owner_orb = split(p, n_orb)
        in_xz = (((x - bx) & 63) < 32) & (((z - bz) & 63) < 32) & (index < count)
        wide = []
        for k in range(4):
            v = terms_ref[owner_orb, owner_slab, 8 * (k % 2) : 8 * (k % 2) + 8, :]
            b = bz if k < 2 else (bz + 32) & 63
            v = jnp.where(z >= b, pltpu.roll(v, b, 1), pltpu.roll(v, (b + 64) & 127, 1))
            wide.append(jnp.where(in_xz, v, 0.0))
        keep = [inside_y(k, by, lane, row) for k in range(4)]
        values = [jnp.where(keep[k], wide[k], 0.0) for k in range(4)]
        values += [jnp.where(keep[k], 0.0, wide[k]) for k in range(4)]
        factors = [jnp.where(both > 0, orb_ref[other, 8 * k : 8 * k + 8, :], 1.0) for k in range(8)]
        return at, [value * factor for value, factor in zip(values, factors)]

    def several(n):
        for at, values in [value_of(TOGETHER * n + k) for k in range(TOGETHER)]:
            for k in range(8):
                out_ref[at, 8 * k : 8 * k + 8, :] = out_ref[at, 8 * k : 8 * k + 8, :] - values[k]

    loop(0, lax.div(count + TOGETHER - 1, TOGETHER), several)


def body(orbitals, pair_list, box_start):
    n_slab, n_orb = lax.axis_size("slab"), lax.axis_size("orb")
    orb_dev, planes, cells = orbitals.shape
    n_pairs = n_slab * n_orb
    slot = (16, 128)
    slots = (n_orb, n_slab) + slot
    rows = orbitals.reshape(orb_dev, planes, cells // 128, 128).transpose(0, 2, 1, 3)
    rows = rows.reshape(orb_dev, planes * cells // 128, 128)
    dma = pltpu.SemaphoreType.DMA
    hbm = pl.BlockSpec(memory_space=pltpu.HBM)
    all_slots, chunked = pltpu.VMEM(slots, F32), pltpu.VMEM((CHUNKS, n_slab // CHUNKS) + slot, F32)
    slabs = pltpu.VMEM((n_slab,) + slot, F32)
    own = jnp.concatenate([pair_list, box_start], axis=1)
    terms, meta, orb_near = pl.pallas_call(
        functools.partial(main_kernel, n_slab, n_orb, orb_dev),
        out_shape=[
            jax.ShapeDtypeStruct(slots, F32),
            jax.ShapeDtypeStruct((n_slab, 1, 128), I32),
            jax.ShapeDtypeStruct(rows.shape, F32),
        ],
        in_specs=[VMEM, hbm],
        out_specs=[VMEM, hbm, VMEM],
        scratch_shapes=[
            pltpu.VMEM((1, 128), I32),
            pltpu.VMEM((n_orb, 1, 128), I32),
            pltpu.VMEM((1, 128), I32),
            pltpu.VMEM((n_slab, 1, 128), I32),
            pltpu.SMEM((n_slab, 1, 128), I32),
            all_slots,
            all_slots,
            chunked,
            chunked,
            slabs,
            slabs,
            pltpu.VMEM((24, 128, 128), F32),
            pltpu.VMEM((24, 48, 128), F32),
            pltpu.VMEM((24, 6, 8, 128), F32),
            pltpu.VMEM((26, 6, 8, 128), F32),
            pltpu.VMEM((26, 6, 8, 128), F32),
            pltpu.VMEM((n_slab // 2,) + slot, F32),
            slabs,
            chunked,
            chunked,
            chunked,
            chunked,
            dma,
            dma((2,)),
            dma((n_orb - 1,)),
            dma((n_orb - 1,)),
            dma((n_slab,)),
            dma((n_slab,)),
            dma((3, 2, CHUNKS)),
            dma((3, 2, CHUNKS)),
            dma((n_slab,)),
            dma((n_slab,)),
            dma((n_slab,)),
            dma((n_slab,)),
        ],
        compiler_params=pltpu.CompilerParams(collective_id=0, has_side_effects=True, vmem_limit_bytes=EXCHANGE_VMEM),
        name="exchange",
    )(own, rows)
    action = pl.pallas_call(
        functools.partial(add_kernel, n_pairs, n_orb, orb_dev),
        out_shape=jax.ShapeDtypeStruct(rows.shape, F32),
        in_specs=[SMEM, VMEM, VMEM],
        out_specs=VMEM,
        scratch_shapes=[pltpu.SMEM((2 * n_pairs + TOGETHER,), I32)],
        compiler_params=pltpu.CompilerParams(vmem_limit_bytes=16 << 20),
        name="add",
    )(meta, terms, orb_near)
    action = action.reshape(orb_dev, cells // 128, planes, 128).transpose(0, 2, 1, 3)
    return action.reshape(orb_dev, planes, cells)


def solution(mesh):
    return jax.shard_map(
        body,
        mesh=mesh,
        in_specs=(P("orb", "slab", None), P(("slab", "orb"), None), P(("slab", "orb"), None)),
        out_specs=P("orb", "slab", None),
        check_vma=False,
    )
```

```python
import functools

import jax
import jax.numpy as jnp
import numpy as np
from jax import lax
from jax.experimental import pallas as pl
from jax.experimental.pallas import tpu as pltpu
from jax.sharding import PartitionSpec as P

ITERS = 16
SCREENING = 0.02
CENTER_EIG = 6.0 + SCREENING
HALF_WIDTH = 6.0

MESH = pl.DeviceIdType.MESH
VMEM = pl.BlockSpec(memory_space=pltpu.VMEM)
SMEM = pl.BlockSpec(memory_space=pltpu.SMEM)
F32 = jnp.float32
I32 = jnp.int32
META = 8
CHUNKS = 4
EXCHANGE_VMEM = 50 << 20
UNROLL = 4
TOGETHER = 4


def chebyshev_weights():
    cheb = np.polynomial.chebyshev
    theta, delta = CENTER_EIG, HALF_WIDTH
    sigma = theta / delta
    potential, residue, update = np.zeros(1), np.ones(1), np.ones(1) / theta
    ratio = 1.0 / sigma
    for _ in range(ITERS):
        potential = cheb.chebadd(potential, update)
        applied = cheb.chebsub(theta * update, 6.0 * cheb.chebmulx(update))
        residue = cheb.chebsub(residue, applied)
        ratio_next = 1.0 / (2.0 * sigma - ratio)
        update = cheb.chebadd(ratio_next * ratio * update, 2.0 * ratio_next / delta * residue)
        ratio = ratio_next
    return [float(c) for c in potential[:ITERS]]


WEIGHTS = chebyshev_weights()


SIDE = 4
FAR_FIRST = (2, 1, 3, 0)
STEPS = ((0, 1), (2, -1), (1, 1), (3, -1))


def peers_at(s, dy):
    y, x = s // (2 * SIDE), (s // 2) % SIDE
    row = 2 * SIDE * ((y + dy) % SIDE)
    found = []
    for dx in FAR_FIRST:
        chip = row + 2 * ((x + dx) % SIDE)
        found += [s ^ 1] if dx == dy == 0 else [chip, chip + 1]
    return found


def peers(s):
    return [q for dy in FAR_FIRST for q in peers_at(s, dy)]


def greet(n_slab, n_orb):
    s, o = lax.axis_index("slab"), lax.axis_index("orb")
    barrier = pltpu.get_barrier_semaphore()
    for q in peers(s):
        pl.semaphore_signal(barrier, 1, device_id={"slab": q}, device_id_type=MESH)
    for d in range(1, n_orb):
        pl.semaphore_signal(barrier, 1, device_id={"orb": lax.rem(o + d, n_orb)}, device_id_type=MESH)

    pl.semaphore_wait(barrier, n_orb - 1 + n_slab - 1)


def remote(src, dst, send, recv, device):
    return pltpu.make_async_remote_copy(
        src_ref=src, dst_ref=dst, send_sem=send, recv_sem=recv, device_id=device, device_id_type=MESH
    )


def lanes_and_rows():
    lane = lax.broadcasted_iota(I32, (8, 128), 1)
    row = lax.broadcasted_iota(I32, (8, 128), 0)
    return lane, row


def inside_y(j, by, lane, row):
    y = 8 * j + 2 * (row >> 1) + (lane >> 6)
    return ((y - by) & 63) < 32


def split(index, count):
    if count & (count - 1):
        return lax.div(index, count), lax.rem(index, count)
    return index >> (count.bit_length() - 1), index & (count - 1)


def pair_of(meta_ref, p, n_orb):
    slab, at = split(p, n_orb)
    return [meta_ref[slab, 0, META * at + k] for k in range(5)]


def loop(low, high, step):
    def run(n, carry):
        step(n)
        return carry

    lax.fori_loop(low, high, run, 0)


def unrolled(low, high, step):
    def run(n, carry):
        step(n)
        return carry

    lax.fori_loop(low, high, run, 0, unroll=UNROLL)


def share(n_slab, n_orb, own_ref, row, trio, joined, meta_v, send_o, recv_o, send_m, recv_m):
    s, o = lax.axis_index("slab"), lax.axis_index("orb")
    row[...] = jnp.zeros((1, 128), I32)
    row[:, 0:5] = own_ref[...]
    line = pltpu.roll(jnp.broadcast_to(row[...], (8, 128)), META * o, 1)[0:1, :]
    row[...] = line
    trio[o] = line
    copies = [
        remote(row, trio.at[o], send_o.at[d - 1], recv_o.at[d - 1], {"orb": lax.rem(o + d, n_orb)})
        for d in range(1, n_orb)
    ]
    for copy in copies:
        copy.start()
    for copy in copies:
        copy.wait()
    total = trio[0]
    for k in range(1, n_orb):
        total = total + trio[k]
    joined[...] = total
    meta_v[s] = total

    def to(q):
        return remote(joined, meta_v.at[s], send_m.at[q], recv_m.at[s], {"slab": q})

    def arrived(q):
        remote(joined, meta_v.at[q], send_m.at[q], recv_m.at[q], {"slab": q}).wait_recv()

    for q in peers(s):
        to(q).start()
    return arrived, lambda q: to(q).wait_send()


def pack_one(n_orb, orb_dev, meta, orb, packed, dest, q):
    o = lax.axis_index("orb")
    lane, row = lanes_and_rows()
    zz = lane & 63
    i, j, _, by, bz = pair_of(meta, q * n_orb + dest, n_orb)
    (oi, li), (oj, lj) = split(i, orb_dev), split(j, orb_dev)
    hold_i, hold_j = oi == o, oj == o
    whole = []
    for k in range(8):
        a = jnp.where(hold_i, orb[li, 8 * k : 8 * k + 8, :], 1.0)
        b = jnp.where(hold_j, orb[lj, 8 * k : 8 * k + 8, :], 1.0)
        whole.append(a * b)
    folded = []
    for k in range(4):
        v = jnp.where(inside_y(k, by, lane, row), whole[k], whole[k + 4])
        b = bz if k < 2 else (bz + 32) & 63
        folded.append(
            jnp.where(zz + b < 64, pltpu.roll(v, (128 - b) & 127, 1), pltpu.roll(v, (64 - b) & 127, 1))
        )
    for k in range(2):
        packed[dest, q, 8 * k : 8 * k + 8, :] = jnp.where(zz < 32, folded[k], folded[k + 2])


def weight_of(index):
    value = jnp.float32(WEIGHTS[0])
    for k in range(1, ITERS):
        value = jnp.where(index == k, jnp.float32(WEIGHTS[k]), value)
    return value


def solve(bx, by, box, out, rows_a, rows_b, source, ping, pong):
    by32 = by & 31
    lane, row = lanes_and_rows()
    zz = lane & 63
    in_z = (zz >= 16) & (zz < 48)

    def place(xm):
        x0, x1 = (bx + xm - 8) & 63, (bx + xm + 16) & 63
        v0 = jnp.where(xm >= 8, box[x0 >> 1, pl.ds(x0 & 1, 8, 2), :], 0.0)
        v1 = jnp.where(xm < 16, box[x1 >> 1, pl.ds(x1 & 1, 8, 2), :], 0.0)
        for h in range(2):
            for q in range(2):
                a = pltpu.roll(v0, (16 - 64 * h - 32 * q) % 128, 1)
                b = pltpu.roll(v1, (80 - 64 * h - 32 * q) % 128, 1)
                v = jnp.where(in_z, jnp.where(lane < 64, a, b), 0.0)
                for dup in range(4):
                    rows_a[xm, pl.ds(32 * dup + 16 * q + h, 8, 2), :] = v

    unrolled(0, 24, place)

    first = WEIGHTS[ITERS - 1]

    def fill(xm):
        for k in range(6):
            u = 6 * row + k - 8
            v = rows_a[xm, pl.ds(by32 + 24 + k, 8, 6), :]
            v = jnp.where((u >= 0) & (u < 32), v, 0.0)
            source[xm, k] = v
            ping[xm + 1, k] = first * v
            pong[xm + 1, k] = jnp.zeros((8, 128), F32)

    unrolled(0, 24, fill)

    def close(ref):
        for k in range(6):
            ref[0, k] = pltpu.roll(ref[24, k], 64, 1)
            ref[25, k] = pltpu.roll(ref[1, k], 64, 1)

    def neighbours(ref, x):
        at = [ref[x, k] for k in range(6)]
        sums = []
        for k in range(6):
            below = at[k - 1] if k > 0 else pltpu.roll(at[5], 1, 0)
            above = at[k + 1] if k < 5 else pltpu.roll(at[0], 7, 0)
            sums.append(
                (ref[x - 1, k] + ref[x + 1, k])
                + (below + above)
                + (pltpu.roll(at[k], 1, 1) + pltpu.roll(at[k], 127, 1))
            )
        return sums

    close(ping)

    def step(now, older, index):
        weight = weight_of(index)
        for xm in range(24):
            sums = neighbours(now, xm + 1)
            for k in range(6):
                older[xm + 1, k] = weight * source[xm, k] + (sums[k] * (1.0 / 3.0) - older[xm + 1, k])
        close(older)

    def two(n):
        step(ping, pong, ITERS - 2 - 2 * n)
        step(pong, ping, ITERS - 3 - 2 * n)

    loop(0, (ITERS - 2) // 2, two)
    weight = WEIGHTS[0]
    for xm in range(24):
        sums = neighbours(ping, xm + 1)
        for k in range(6):
            rows_b[xm, pl.ds(k, 8, 6), :] = weight * source[xm, k] + (sums[k] * (1.0 / 6.0) - pong[xm + 1, k])

    def twice(xm):
        for m in range(4):
            v = rows_b[xm, 8 + 8 * m : 16 + 8 * m, :]
            rows_a[xm, 8 * m : 8 * m + 8, :] = v
            rows_a[xm, 32 + 8 * m : 40 + 8 * m, :] = v

    unrolled(0, 24, twice)

    def give(x2):
        for plane in range(2):
            ux = (2 * x2 + plane - bx) & 31
            half = (ux >= 16).astype(I32)
            xm = ux + 8 - 24 * half
            pieces = []
            for h in range(2):
                for q in range(2):
                    v = rows_a[xm, pl.ds(32 - by32 + 16 * q + h, 8, 2), :]
                    pieces.append(pltpu.roll(v, (64 * h + 32 * q - 16 + 128 - 64 * half) & 127, 1))
            v = jnp.where(
                lane < 64,
                jnp.where(zz < 32, pieces[0], pieces[1]),
                jnp.where(zz < 32, pieces[2], pieces[3]),
            )
            out[x2, pl.ds(plane, 8, 2), :] = v

    unrolled(0, 16, give)


def main_kernel(
    n_slab, n_orb, orb_dev, own_ref, orb_hbm, terms, meta_hbm, orb,
    row, trio, joined, meta_v, meta_s, packed, held, relay, combined, density, box,
    rows_a, rows_b, source, ping, pong, potential, mine, to_relay, to_plain, to_far, from_dest,
    load_sem, meta_sem, send_o, recv_o, send_m, recv_m, ring_sem, back_sem, send_d, recv_d, send_p, recv_p,
):
    s, o = lax.axis_index("slab"), lax.axis_index("orb")
    half, size = n_slab // 2, n_slab // CHUNKS
    load = pltpu.make_async_copy(orb_hbm, orb, load_sem)
    load.start()
    greet(n_slab, n_orb)
    row_arrived, row_sent = share(
        n_slab, n_orb, own_ref, row, trio, joined, meta_v, send_o, recv_o, send_m, recv_m
    )

    chunks = [(lax.rem(lax.div(s, size) + k, CHUNKS), way) for k, way in STEPS]

    def plane(d):
        return lax.rem(o + d + n_orb, n_orb)

    def rows(c):
        return pl.ds(c * size, size)

    def chunk_loop(c, step):
        unrolled(0, size, lambda n: step(c * size + n, n))

    def ring_copy(kind, sems, source, target, c, d):
        return remote(source, target, sems.at[kind, 0, c], sems.at[kind, 1, c], {"orb": plane(d)})

    def far(c, way):
        return ring_copy(0, ring_sem, packed.at[plane(2), rows(c)], relay.at[c], c, way)

    def through(c, way):
        return ring_copy(1, ring_sem, combined.at[c], held.at[o, rows(c)], c, way)

    def straight(c, way):
        return ring_copy(2, ring_sem, packed.at[plane(-way), rows(c)], held.at[o, rows(c)], c, -way)

    def pack(d, c, into):
        dest = plane(d)
        chunk_loop(c, lambda q, n: pack_one(n_orb, orb_dev, meta_s, orb, into, dest, q))

    def pass_on(c, way):
        far(c, way).wait_recv()

        def step(q, n):
            combined[c, n] = relay[c, n] * packed[plane(way), q]

        chunk_loop(c, step)
        through(c, way).start()

    for at, (c, way) in enumerate(chunks):
        for q in peers_at(s, STEPS[at][0]):
            row_arrived(q)
        local = pltpu.make_async_copy(meta_v.at[rows(c)], meta_s.at[rows(c)], meta_sem.at[0])
        local.start()
        local.wait()
        if at == 0:
            load.wait()
        pack(2, c, packed)
        far(c, way).start()
    keep = pltpu.make_async_copy(meta_v, meta_hbm, meta_sem.at[1])
    keep.start()
    for c, way in chunks:
        pack(-way, c, packed)
        straight(c, way).start()
    for c, way in chunks:
        pack(way, c, packed)
        pass_on(c, way)
    for c, _ in chunks:
        pack(0, c, held)

    def to_owner(q):
        return remote(density.at[q], box.at[s], send_d.at[q], recv_d.at[s], {"slab": q})

    def from_slab(q):
        return remote(density.at[q], box.at[q], send_d.at[q], recv_d.at[q], {"slab": q})

    for at, (c, way) in enumerate(chunks):
        through(c, way).wait_recv()
        straight(c, way).wait_recv()

        def form(q, n):
            density[q] = held[o, q] * (held[plane(1), q] * held[plane(-1), q])

        chunk_loop(c, form)
        for q in peers_at(s, STEPS[at][0]):
            to_owner(q).start()
    box[s] = density[s]
    for q in peers(s):
        from_slab(q).wait_recv()

    _, _, bx, by, _ = pair_of(meta_s, s * n_orb + o, n_orb)
    solve(bx, by, box, potential, rows_a, rows_b, source, ping, pong)

    def to_slab(q):
        return remote(potential.at[lax.rem(q, half)], mine.at[s], send_p.at[q], recv_p.at[s], {"slab": q})

    def from_owner(q):
        return remote(potential.at[lax.rem(q, half)], mine.at[q], send_p.at[q], recv_p.at[q], {"slab": q})

    for k, _ in STEPS:
        for q in peers_at(s, k):
            to_slab(q).start()
    mine[s] = potential[lax.rem(s, half)]

    def back_relay(c, way):
        return ring_copy(0, back_sem, to_relay.at[c], from_dest.at[c], c, -way)

    def back_straight(c, way):
        return ring_copy(1, back_sem, to_plain.at[c], terms.at[o, rows(c)], c, way)

    def back_far(c, way):
        return ring_copy(2, back_sem, to_far.at[c], terms.at[plane(way), rows(c)], c, -way)

    def finish(c, way):
        back_relay(c, way).wait_recv()

        def step(q, n):
            value = from_dest[c, n]
            to_far[c, n] = value * packed[plane(way), q]
            terms[plane(way), q] = value * relay[c, n]

        chunk_loop(c, step)
        back_far(c, way).start()

    for at, (c, way) in enumerate(chunks):
        for q in peers_at(s, STEPS[at][0]):
            from_owner(q).wait_recv()

        def share_out(q, n):
            own = mine[q] * held[o, q]
            to_relay[c, n] = own * held[plane(way), q]
            to_plain[c, n] = own * held[plane(-way), q]

        chunk_loop(c, share_out)
        back_relay(c, way).start()
        back_straight(c, way).start()
    for c, way in chunks:
        finish(c, way)
    for c, _ in chunks:

        def own_term(q, n):
            terms[o, q] = mine[q] * (held[plane(1), q] * held[plane(-1), q])

        chunk_loop(c, own_term)
    for c, way in chunks:
        back_straight(c, way).wait_recv()
        back_far(c, way).wait_recv()
    for c, way in chunks:
        for copy in (far, through, straight, back_relay, back_straight, back_far):
            copy(c, way).wait_send()

    for q in peers(s):
        row_sent(q)
        to_owner(q).wait_send()
        to_slab(q).wait_send()
    keep.wait()


def add_kernel(n_pairs, n_orb, orb_dev, meta_ref, terms_ref, orb_ref, out_ref, entries):
    s, o = lax.axis_index("slab"), lax.axis_index("orb")
    lane, row = lanes_and_rows()
    z = lane & 63
    x = 2 * s + (row & 1)
    clear = out_ref.shape[1] * orb_dev // n_pairs

    def collect(p, count):
        i, j = pair_of(meta_ref, p, n_orb)[:2]
        (oi, li), (oj, lj) = split(i, orb_dev), split(j, orb_dev)
        both = (oi == oj).astype(I32) * orb_dev
        entries[count] = ((both + lj) * orb_dev + li) * n_pairs + p
        count = count + (oi == o).astype(I32)
        entries[count] = ((both + li) * orb_dev + lj) * n_pairs + p
        count = count + (oj == o).astype(I32)
        at, part = split(p, n_pairs // orb_dev)
        out_ref[at, pl.ds(pl.multiple_of(part * clear, clear), clear), :] = jnp.zeros((clear, 128), F32)
        return count

    count = lax.fori_loop(0, n_pairs, collect, 0, unroll=UNROLL)
    for k in range(TOGETHER):
        entries[count + k] = 0

    def value_of(index):
        rest, p = split(entries[index], n_pairs)
        rest, at = split(rest, orb_dev)
        both, other = split(rest, orb_dev)
        _, _, bx, by, bz = pair_of(meta_ref, p, n_orb)
        owner_slab, owner_orb = split(p, n_orb)
        in_xz = (((x - bx) & 63) < 32) & (((z - bz) & 63) < 32) & (index < count)
        wide = []
        for k in range(4):
            v = terms_ref[owner_orb, owner_slab, 8 * (k % 2) : 8 * (k % 2) + 8, :]
            b = bz if k < 2 else (bz + 32) & 63
            v = jnp.where(z >= b, pltpu.roll(v, b, 1), pltpu.roll(v, (b + 64) & 127, 1))
            wide.append(jnp.where(in_xz, v, 0.0))
        keep = [inside_y(k, by, lane, row) for k in range(4)]
        values = [jnp.where(keep[k], wide[k], 0.0) for k in range(4)]
        values += [jnp.where(keep[k], 0.0, wide[k]) for k in range(4)]
        factors = [jnp.where(both > 0, orb_ref[other, 8 * k : 8 * k + 8, :], 1.0) for k in range(8)]
        return at, [value * factor for value, factor in zip(values, factors)]

    def several(n):
        for at, values in [value_of(TOGETHER * n + k) for k in range(TOGETHER)]:
            for k in range(8):
                out_ref[at, 8 * k : 8 * k + 8, :] = out_ref[at, 8 * k : 8 * k + 8, :] - values[k]

    loop(0, lax.div(count + TOGETHER - 1, TOGETHER), several)


def body(orbitals, pair_list, box_start):
    n_slab, n_orb = lax.axis_size("slab"), lax.axis_size("orb")
    orb_dev, planes, cells = orbitals.shape
    n_pairs = n_slab * n_orb
    slot = (16, 128)
    slots = (n_orb, n_slab) + slot
    rows = orbitals.reshape(orb_dev, planes, cells // 128, 128).transpose(0, 2, 1, 3)
    rows = rows.reshape(orb_dev, planes * cells // 128, 128)
    dma = pltpu.SemaphoreType.DMA
    hbm = pl.BlockSpec(memory_space=pltpu.HBM)
    all_slots, chunked = pltpu.VMEM(slots, F32), pltpu.VMEM((CHUNKS, n_slab // CHUNKS) + slot, F32)
    slabs = pltpu.VMEM((n_slab,) + slot, F32)
    own = jnp.concatenate([pair_list, box_start], axis=1)
    terms, meta, orb_near = pl.pallas_call(
        functools.partial(main_kernel, n_slab, n_orb, orb_dev),
        out_shape=[
            jax.ShapeDtypeStruct(slots, F32),
            jax.ShapeDtypeStruct((n_slab, 1, 128), I32),
            jax.ShapeDtypeStruct(rows.shape, F32),
        ],
        in_specs=[VMEM, hbm],
        out_specs=[VMEM, hbm, VMEM],
        scratch_shapes=[
            pltpu.VMEM((1, 128), I32),
            pltpu.VMEM((n_orb, 1, 128), I32),
            pltpu.VMEM((1, 128), I32),
            pltpu.VMEM((n_slab, 1, 128), I32),
            pltpu.SMEM((n_slab, 1, 128), I32),
            all_slots,
            all_slots,
            chunked,
            chunked,
            slabs,
            slabs,
            pltpu.VMEM((24, 128, 128), F32),
            pltpu.VMEM((24, 48, 128), F32),
            pltpu.VMEM((24, 6, 8, 128), F32),
            pltpu.VMEM((26, 6, 8, 128), F32),
            pltpu.VMEM((26, 6, 8, 128), F32),
            pltpu.VMEM((n_slab // 2,) + slot, F32),
            slabs,
            chunked,
            chunked,
            chunked,
            chunked,
            dma,
            dma((2,)),
            dma((n_orb - 1,)),
            dma((n_orb - 1,)),
            dma((n_slab,)),
            dma((n_slab,)),
            dma((3, 2, CHUNKS)),
            dma((3, 2, CHUNKS)),
            dma((n_slab,)),
            dma((n_slab,)),
            dma((n_slab,)),
            dma((n_slab,)),
        ],
        compiler_params=pltpu.CompilerParams(collective_id=0, has_side_effects=True, vmem_limit_bytes=EXCHANGE_VMEM),
        name="exchange",
    )(own, rows)
    action = pl.pallas_call(
        functools.partial(add_kernel, n_pairs, n_orb, orb_dev),
        out_shape=jax.ShapeDtypeStruct(rows.shape, F32),
        in_specs=[SMEM, VMEM, VMEM],
        out_specs=VMEM,
        scratch_shapes=[pltpu.SMEM((2 * n_pairs + TOGETHER,), I32)],
        compiler_params=pltpu.CompilerParams(vmem_limit_bytes=16 << 20),
        name="add",
    )(meta, terms, orb_near)
    action = action.reshape(orb_dev, cells // 128, planes, 128).transpose(0, 2, 1, 3)
    return action.reshape(orb_dev, planes, cells)


def solution(mesh):
    return jax.shard_map(
        body,
        mesh=mesh,
        in_specs=(P("orb", "slab", None), P(("slab", "orb"), None), P(("slab", "orb"), None)),
        out_specs=P("orb", "slab", None),
        check_vma=False,
    )
```

```python
import functools

import jax
import jax.numpy as jnp
import numpy as np
from jax import lax
from jax.experimental import pallas as pl
from jax.experimental.pallas import tpu as pltpu
from jax.sharding import PartitionSpec as P

ITERS = 16
SCREENING = 0.02
CENTER_EIG = 6.0 + SCREENING
HALF_WIDTH = 6.0

MESH = pl.DeviceIdType.MESH
VMEM = pl.BlockSpec(memory_space=pltpu.VMEM)
SMEM = pl.BlockSpec(memory_space=pltpu.SMEM)
F32 = jnp.float32
I32 = jnp.int32
META = 8
CHUNKS = 4
EXCHANGE_VMEM = 50 << 20
UNROLL = 4
TOGETHER = 4


def chebyshev_weights():
    cheb = np.polynomial.chebyshev
    theta, delta = CENTER_EIG, HALF_WIDTH
    sigma = theta / delta
    potential, residue, update = np.zeros(1), np.ones(1), np.ones(1) / theta
    ratio = 1.0 / sigma
    for _ in range(ITERS):
        potential = cheb.chebadd(potential, update)
        applied = cheb.chebsub(theta * update, 6.0 * cheb.chebmulx(update))
        residue = cheb.chebsub(residue, applied)
        ratio_next = 1.0 / (2.0 * sigma - ratio)
        update = cheb.chebadd(ratio_next * ratio * update, 2.0 * ratio_next / delta * residue)
        ratio = ratio_next
    return [float(c) for c in potential[:ITERS]]


WEIGHTS = chebyshev_weights()


SIDE = 4
FAR_FIRST = (2, 1, 3, 0)
STEPS = ((0, 1), (2, -1), (1, 1), (3, -1))
NEAR_LAST = (1, 2, 3, 0)


def peers_at(s, dy):
    y, x = s // (2 * SIDE), (s // 2) % SIDE
    row = 2 * SIDE * ((y + dy) % SIDE)
    found = []
    for dx in FAR_FIRST:
        chip = row + 2 * ((x + dx) % SIDE)
        found += [s ^ 1] if dx == dy == 0 else [chip, chip + 1]
    return found


def peers(s):
    return [q for dy in FAR_FIRST for q in peers_at(s, dy)]


def greet(n_slab, n_orb, meanwhile):
    s, o = lax.axis_index("slab"), lax.axis_index("orb")
    barrier = pltpu.get_barrier_semaphore()
    for q in peers(s):
        pl.semaphore_signal(barrier, 1, device_id={"slab": q}, device_id_type=MESH)
    for d in range(1, n_orb):
        pl.semaphore_signal(barrier, 1, device_id={"orb": lax.rem(o + d, n_orb)}, device_id_type=MESH)

    meanwhile()
    pl.semaphore_wait(barrier, n_orb - 1 + n_slab - 1)


def remote(src, dst, send, recv, device):
    return pltpu.make_async_remote_copy(
        src_ref=src, dst_ref=dst, send_sem=send, recv_sem=recv, device_id=device, device_id_type=MESH
    )


def lanes_and_rows():
    lane = lax.broadcasted_iota(I32, (8, 128), 1)
    row = lax.broadcasted_iota(I32, (8, 128), 0)
    return lane, row


def inside_y(j, by, lane, row):
    y = 8 * j + 2 * (row >> 1) + (lane >> 6)
    return ((y - by) & 63) < 32


def split(index, count):
    if count & (count - 1):
        return lax.div(index, count), lax.rem(index, count)
    return index >> (count.bit_length() - 1), index & (count - 1)


def pair_of(meta_ref, p, n_orb):
    slab, at = split(p, n_orb)
    return [meta_ref[slab, 0, META * at + k] for k in range(5)]


def loop(low, high, step):
    def run(n, carry):
        step(n)
        return carry

    lax.fori_loop(low, high, run, 0)


def unrolled(low, high, step):
    def run(n, carry):
        step(n)
        return carry

    lax.fori_loop(low, high, run, 0, unroll=UNROLL)


def share(n_slab, n_orb, own_ref, row, trio, joined, meta_v, send_o, recv_o, send_m, recv_m):
    s, o = lax.axis_index("slab"), lax.axis_index("orb")
    row[...] = jnp.zeros((1, 128), I32)
    row[:, 0:5] = own_ref[...]
    line = pltpu.roll(jnp.broadcast_to(row[...], (8, 128)), META * o, 1)[0:1, :]
    row[...] = line
    trio[o] = line
    copies = [
        remote(row, trio.at[o], send_o.at[d - 1], recv_o.at[d - 1], {"orb": lax.rem(o + d, n_orb)})
        for d in range(1, n_orb)
    ]
    for copy in copies:
        copy.start()
    for copy in copies:
        copy.wait()
    total = trio[0]
    for k in range(1, n_orb):
        total = total + trio[k]
    joined[...] = total
    meta_v[s] = total

    def to(q):
        return remote(joined, meta_v.at[s], send_m.at[q], recv_m.at[s], {"slab": q})

    def arrived(q):
        remote(joined, meta_v.at[q], send_m.at[q], recv_m.at[q], {"slab": q}).wait_recv()

    for q in peers(s):
        to(q).start()
    return arrived, lambda q: to(q).wait_send()


def pack_one(n_orb, orb_dev, meta, orb, packed, dest, q):
    o = lax.axis_index("orb")
    lane, row = lanes_and_rows()
    zz = lane & 63
    i, j, _, by, bz = pair_of(meta, q * n_orb + dest, n_orb)
    (oi, li), (oj, lj) = split(i, orb_dev), split(j, orb_dev)
    hold_i, hold_j = oi == o, oj == o
    whole = []
    for k in range(8):
        a = jnp.where(hold_i, orb[li, 8 * k : 8 * k + 8, :], 1.0)
        b = jnp.where(hold_j, orb[lj, 8 * k : 8 * k + 8, :], 1.0)
        whole.append(a * b)
    folded = []
    for k in range(4):
        v = jnp.where(inside_y(k, by, lane, row), whole[k], whole[k + 4])
        b = bz if k < 2 else (bz + 32) & 63
        folded.append(
            jnp.where(zz + b < 64, pltpu.roll(v, (128 - b) & 127, 1), pltpu.roll(v, (64 - b) & 127, 1))
        )
    for k in range(2):
        packed[dest, q, 8 * k : 8 * k + 8, :] = jnp.where(zz < 32, folded[k], folded[k + 2])


def weight_of(index):
    value = jnp.float32(WEIGHTS[0])
    for k in range(1, ITERS):
        value = jnp.where(index == k, jnp.float32(WEIGHTS[k]), value)
    return value


def cosines(index):
    turn = index & 63
    turn = jnp.minimum(turn, 64 - turn)
    value = jnp.full(index.shape, 1.0, F32)
    for k in range(1, 33):
        value = jnp.where(turn == k, float(np.cos(2.0 * np.pi * k / 64.0)), value)
    return value


def mode_of(m):
    wave = jnp.where(m <= 32, m, m - 32)
    norm = jnp.where((m == 0) | (m == 32), 0.125, 0.125 * float(np.sqrt(2.0)))
    return wave, jnp.where(m <= 32, 0, 16), norm


def modes(to_modes, from_modes, eigen):
    lane, row = lanes_and_rows()
    mode, cell, group = lane & 63, lane & 31, lane >> 5
    wave, quarter, norm = mode_of(mode)
    eigen[...] = (2.0 / 3.0) * cosines(wave)
    zero = jnp.zeros((8, 128), F32)
    for r in range(4):
        table = norm * cosines(wave * (8 * r + row) - quarter)
        for half in range(2):
            part = jnp.where((lane >> 6) == half, table, 0.0)
            for g in range(4):
                top = 128 * half + 32 * g + 8 * r
                for other in range(4):
                    to_modes[top : top + 8, 128 * other : 128 * other + 128] = part if other == g else zero
    for r in range(8):
        wave, quarter, norm = mode_of(8 * r + row)
        table = norm * cosines(wave * cell - quarter)
        for g in range(4):
            part = jnp.where(group == g, table, 0.0)
            for half in range(2):
                top = 128 * g + 64 * half + 8 * r
                for other in range(2):
                    from_modes[top : top + 8, 128 * other : 128 * other + 128] = part if other == half else zero


def exact_dot(a, b):
    return jnp.dot(a, b, precision=lax.Precision.HIGHEST, preferred_element_type=F32)


def solve(bx, by, box, out, rows_a, rows_b, source, ping, pong, to_modes, from_modes, eigen, pairs, wide, halves):
    by32 = by & 31
    lane, row = lanes_and_rows()

    def place(xm):
        x0, x1 = (bx + xm - 8) & 63, (bx + xm + 16) & 63
        at = pl.ds(pl.multiple_of(8 * xm, 8), 8)
        pairs[at, 0:128] = jnp.where(xm >= 8, box[x0 >> 1, pl.ds(x0 & 1, 8, 2), :], 0.0)
        pairs[at, 128:256] = jnp.where(xm < 16, box[x1 >> 1, pl.ds(x1 & 1, 8, 2), :], 0.0)

    unrolled(0, 24, place)
    wide[...] = exact_dot(pairs[...], to_modes[...])

    def spread(xm):
        at = pl.ds(pl.multiple_of(8 * xm, 8), 8)
        for h in range(2):
            for q in range(2):
                g = 2 * h + q
                v = wide[at, 128 * g : 128 * g + 128]
                for dup in range(4):
                    rows_a[xm, pl.ds(32 * dup + 16 * q + h, 8, 2), :] = v

    unrolled(0, 24, spread)

    first = WEIGHTS[ITERS - 1]

    def fill(xm):
        for k in range(6):
            u = 6 * row + k - 8
            v = rows_a[xm, pl.ds(by32 + 24 + k, 8, 6), :]
            v = jnp.where((u >= 0) & (u < 32), v, 0.0)
            source[xm, k] = v
            ping[xm + 1, k] = first * v
            pong[xm + 1, k] = jnp.zeros((8, 128), F32)

    unrolled(0, 24, fill)

    def close(ref):
        for k in range(6):
            ref[0, k] = pltpu.roll(ref[24, k], 64, 1)
            ref[25, k] = pltpu.roll(ref[1, k], 64, 1)

    along_z = eigen[...]

    def doubled(ref, x, at, before, after):
        values = []
        for k in range(6):
            below = at[k - 1] if k > 0 else pltpu.roll(at[5], 1, 0)
            above = at[k + 1] if k < 5 else pltpu.roll(at[0], 7, 0)
            values.append(((before[k] + after[k]) + (below + above)) * (1.0 / 3.0) + along_z * at[k])
        return values

    def sweep(now, finish):
        column = lambda x: [now[x, k] for k in range(6)]
        before, at = column(0), column(1)
        for xm in range(24):
            after = column(xm + 2)
            finish(xm, doubled(now, xm + 1, at, before, after))
            before, at = at, after

    close(ping)

    def step(now, older, index):
        weight = weight_of(index)

        def finish(xm, values):
            for k in range(6):
                older[xm + 1, k] = weight * source[xm, k] + (values[k] - older[xm + 1, k])

        sweep(now, finish)
        close(older)

    def two(n):
        step(ping, pong, ITERS - 2 - 2 * n)
        step(pong, ping, ITERS - 3 - 2 * n)

    loop(0, (ITERS - 2) // 2, two)

    def last(xm, values):
        for k in range(6):
            rows_b[xm, pl.ds(k, 8, 6), :] = WEIGHTS[0] * source[xm, k] + (values[k] * 0.5 - pong[xm + 1, k])

    sweep(ping, last)

    def twice(xm):
        for m in range(4):
            v = rows_b[xm, 8 + 8 * m : 16 + 8 * m, :]
            rows_a[xm, 8 * m : 8 * m + 8, :] = v
            rows_a[xm, 32 + 8 * m : 40 + 8 * m, :] = v

    unrolled(0, 24, twice)

    def collect(xm):
        at = pl.ds(pl.multiple_of(8 * xm, 8), 8)
        for h in range(2):
            for q in range(2):
                g = 2 * h + q
                wide[at, 128 * g : 128 * g + 128] = rows_a[xm, pl.ds(32 - by32 + 16 * q + h, 8, 2), :]

    unrolled(0, 24, collect)
    both = exact_dot(wide[...], from_modes[...])
    for half in range(2):
        halves[:, half] = both[:, 128 * half : 128 * half + 128].reshape(24, 8, 128)

    def give(x2):
        for plane in range(2):
            ux = (2 * x2 + plane - bx) & 31
            half = (ux >= 16).astype(I32)
            xm = ux + 8 - 24 * half
            out[x2, pl.ds(plane, 8, 2), :] = jnp.where(half == 0, halves[xm, 0], halves[xm, 1])

    unrolled(0, 16, give)


def main_kernel(
    n_slab, n_orb, orb_dev, own_ref, orb_hbm, terms, meta_hbm, orb,
    row, trio, joined, meta_v, meta_s, packed, held, relay, combined, density, box,
    rows_a, rows_b, source, ping, pong, to_modes, from_modes, eigen, joint, wide, halves, potential, mine, to_relay, to_plain, to_far, from_dest,
    load_sem, meta_sem, send_o, recv_o, send_m, recv_m, ring_sem, back_sem, send_d, recv_d, send_p, recv_p,
):
    s, o = lax.axis_index("slab"), lax.axis_index("orb")
    half, size = n_slab // 2, n_slab // CHUNKS
    load = pltpu.make_async_copy(orb_hbm, orb, load_sem)
    load.start()
    greet(n_slab, n_orb, lambda: modes(to_modes, from_modes, eigen))
    row_arrived, row_sent = share(
        n_slab, n_orb, own_ref, row, trio, joined, meta_v, send_o, recv_o, send_m, recv_m
    )

    chunks = [(lax.rem(lax.div(s, size) + k, CHUNKS), way) for k, way in STEPS]

    def plane(d):
        return lax.rem(o + d + n_orb, n_orb)

    def rows(c):
        return pl.ds(c * size, size)

    def chunk_loop(c, step):
        unrolled(0, size, lambda n: step(c * size + n, n))

    def ring_copy(kind, sems, source, target, c, d):
        return remote(source, target, sems.at[kind, 0, c], sems.at[kind, 1, c], {"orb": plane(d)})

    def far(c, way):
        return ring_copy(0, ring_sem, packed.at[plane(2), rows(c)], relay.at[c], c, way)

    def through(c, way):
        return ring_copy(1, ring_sem, combined.at[c], held.at[o, rows(c)], c, way)

    def straight(c, way):
        return ring_copy(2, ring_sem, packed.at[plane(-way), rows(c)], held.at[o, rows(c)], c, -way)

    def pack(d, c, into):
        dest = plane(d)
        chunk_loop(c, lambda q, n: pack_one(n_orb, orb_dev, meta_s, orb, into, dest, q))

    def pass_on(c, way):
        far(c, way).wait_recv()

        def step(q, n):
            combined[c, n] = relay[c, n] * packed[plane(way), q]

        chunk_loop(c, step)
        through(c, way).start()

    for at, (c, way) in enumerate(chunks):
        for q in peers_at(s, STEPS[at][0]):
            row_arrived(q)
        local = pltpu.make_async_copy(meta_v.at[rows(c)], meta_s.at[rows(c)], meta_sem.at[0])
        local.start()
        local.wait()
        if at == 0:
            load.wait()
        pack(2, c, packed)
        far(c, way).start()
    keep = pltpu.make_async_copy(meta_v, meta_hbm, meta_sem.at[1])
    keep.start()
    for at in NEAR_LAST:
        c, way = chunks[at]
        pack(-way, c, packed)
        straight(c, way).start()
    for at in NEAR_LAST:
        c, way = chunks[at]
        pack(way, c, packed)
        pass_on(c, way)
    for c, _ in chunks:
        pack(0, c, held)

    def to_owner(q):
        return remote(density.at[q], box.at[s], send_d.at[q], recv_d.at[s], {"slab": q})

    def from_slab(q):
        return remote(density.at[q], box.at[q], send_d.at[q], recv_d.at[q], {"slab": q})

    for at in NEAR_LAST:
        c, way = chunks[at]
        through(c, way).wait_recv()
        straight(c, way).wait_recv()

        def form(q, n):
            density[q] = held[o, q] * (held[plane(1), q] * held[plane(-1), q])

        chunk_loop(c, form)
        for q in peers_at(s, STEPS[at][0]):
            to_owner(q).start()
    box[s] = density[s]
    for q in peers(s):
        from_slab(q).wait_recv()

    _, _, bx, by, _ = pair_of(meta_s, s * n_orb + o, n_orb)
    solve(bx, by, box, potential, rows_a, rows_b, source, ping, pong, to_modes, from_modes, eigen, joint, wide, halves)

    def to_slab(q):
        return remote(potential.at[lax.rem(q, half)], mine.at[s], send_p.at[q], recv_p.at[s], {"slab": q})

    def from_owner(q):
        return remote(potential.at[lax.rem(q, half)], mine.at[q], send_p.at[q], recv_p.at[q], {"slab": q})

    for k, _ in STEPS:
        for q in peers_at(s, k):
            to_slab(q).start()
    mine[s] = potential[lax.rem(s, half)]

    def back_relay(c, way):
        return ring_copy(0, back_sem, to_relay.at[c], from_dest.at[c], c, -way)

    def back_straight(c, way):
        return ring_copy(1, back_sem, to_plain.at[c], terms.at[o, rows(c)], c, way)

    def back_far(c, way):
        return ring_copy(2, back_sem, to_far.at[c], terms.at[plane(way), rows(c)], c, -way)

    def finish(c, way):
        back_relay(c, way).wait_recv()

        def step(q, n):
            value = from_dest[c, n]
            to_far[c, n] = value * packed[plane(way), q]
            terms[plane(way), q] = value * relay[c, n]

        chunk_loop(c, step)
        back_far(c, way).start()

    for at, (c, way) in enumerate(chunks):
        for q in peers_at(s, STEPS[at][0]):
            from_owner(q).wait_recv()

        def share_out(q, n):
            own = mine[q] * held[o, q]
            to_relay[c, n] = own * held[plane(way), q]
            to_plain[c, n] = own * held[plane(-way), q]

        chunk_loop(c, share_out)
        back_relay(c, way).start()
        back_straight(c, way).start()
    for c, way in chunks:
        finish(c, way)
    for c, _ in chunks:

        def own_term(q, n):
            terms[o, q] = mine[q] * (held[plane(1), q] * held[plane(-1), q])

        chunk_loop(c, own_term)
    for c, way in chunks:
        back_straight(c, way).wait_recv()
        back_far(c, way).wait_recv()
    for c, way in chunks:
        for copy in (far, through, straight, back_relay, back_straight, back_far):
            copy(c, way).wait_send()

    for q in peers(s):
        row_sent(q)
        to_owner(q).wait_send()
        to_slab(q).wait_send()
    keep.wait()


def add_kernel(n_pairs, n_orb, orb_dev, meta_ref, terms_ref, orb_ref, out_ref, entries):
    s, o = lax.axis_index("slab"), lax.axis_index("orb")
    lane, row = lanes_and_rows()
    z = lane & 63
    x = 2 * s + (row & 1)
    clear = out_ref.shape[1] * orb_dev // n_pairs

    def collect(p, count):
        i, j = pair_of(meta_ref, p, n_orb)[:2]
        (oi, li), (oj, lj) = split(i, orb_dev), split(j, orb_dev)
        both = (oi == oj).astype(I32) * orb_dev
        entries[count] = ((both + lj) * orb_dev + li) * n_pairs + p
        count = count + (oi == o).astype(I32)
        entries[count] = ((both + li) * orb_dev + lj) * n_pairs + p
        count = count + (oj == o).astype(I32)
        at, part = split(p, n_pairs // orb_dev)
        out_ref[at, pl.ds(pl.multiple_of(part * clear, clear), clear), :] = jnp.zeros((clear, 128), F32)
        return count

    count = lax.fori_loop(0, n_pairs, collect, 0, unroll=UNROLL)
    for k in range(TOGETHER):
        entries[count + k] = 0

    def value_of(index):
        rest, p = split(entries[index], n_pairs)
        rest, at = split(rest, orb_dev)
        both, other = split(rest, orb_dev)
        _, _, bx, by, bz = pair_of(meta_ref, p, n_orb)
        owner_slab, owner_orb = split(p, n_orb)
        in_xz = (((x - bx) & 63) < 32) & (((z - bz) & 63) < 32) & (index < count)
        wide = []
        for k in range(4):
            v = terms_ref[owner_orb, owner_slab, 8 * (k % 2) : 8 * (k % 2) + 8, :]
            b = bz if k < 2 else (bz + 32) & 63
            v = jnp.where(z >= b, pltpu.roll(v, b, 1), pltpu.roll(v, (b + 64) & 127, 1))
            wide.append(jnp.where(in_xz, v, 0.0))
        keep = [inside_y(k, by, lane, row) for k in range(4)]
        values = [jnp.where(keep[k], wide[k], 0.0) for k in range(4)]
        values += [jnp.where(keep[k], 0.0, wide[k]) for k in range(4)]
        factors = [jnp.where(both > 0, orb_ref[other, 8 * k : 8 * k + 8, :], 1.0) for k in range(8)]
        return at, [value * factor for value, factor in zip(values, factors)]

    def several(n):
        for at, values in [value_of(TOGETHER * n + k) for k in range(TOGETHER)]:
            for k in range(8):
                out_ref[at, 8 * k : 8 * k + 8, :] = out_ref[at, 8 * k : 8 * k + 8, :] - values[k]

    loop(0, lax.div(count + TOGETHER - 1, TOGETHER), several)


def body(orbitals, pair_list, box_start):
    n_slab, n_orb = lax.axis_size("slab"), lax.axis_size("orb")
    orb_dev, planes, cells = orbitals.shape
    n_pairs = n_slab * n_orb
    slot = (16, 128)
    slots = (n_orb, n_slab) + slot
    rows = orbitals.reshape(orb_dev, planes, cells // 128, 128).transpose(0, 2, 1, 3)
    rows = rows.reshape(orb_dev, planes * cells // 128, 128)
    dma = pltpu.SemaphoreType.DMA
    hbm = pl.BlockSpec(memory_space=pltpu.HBM)
    all_slots, chunked = pltpu.VMEM(slots, F32), pltpu.VMEM((CHUNKS, n_slab // CHUNKS) + slot, F32)
    slabs = pltpu.VMEM((n_slab,) + slot, F32)
    own = jnp.concatenate([pair_list, box_start], axis=1)
    terms, meta, orb_near = pl.pallas_call(
        functools.partial(main_kernel, n_slab, n_orb, orb_dev),
        out_shape=[
            jax.ShapeDtypeStruct(slots, F32),
            jax.ShapeDtypeStruct((n_slab, 1, 128), I32),
            jax.ShapeDtypeStruct(rows.shape, F32),
        ],
        in_specs=[VMEM, hbm],
        out_specs=[VMEM, hbm, VMEM],
        scratch_shapes=[
            pltpu.VMEM((1, 128), I32),
            pltpu.VMEM((n_orb, 1, 128), I32),
            pltpu.VMEM((1, 128), I32),
            pltpu.VMEM((n_slab, 1, 128), I32),
            pltpu.SMEM((n_slab, 1, 128), I32),
            all_slots,
            all_slots,
            chunked,
            chunked,
            slabs,
            slabs,
            pltpu.VMEM((24, 128, 128), F32),
            pltpu.VMEM((24, 48, 128), F32),
            pltpu.VMEM((24, 6, 8, 128), F32),
            pltpu.VMEM((26, 6, 8, 128), F32),
            pltpu.VMEM((26, 6, 8, 128), F32),
            pltpu.VMEM((256, 512), F32),
            pltpu.VMEM((512, 256), F32),
            pltpu.VMEM((8, 128), F32),
            pltpu.VMEM((192, 256), F32),
            pltpu.VMEM((192, 512), F32),
            pltpu.VMEM((24, 2, 8, 128), F32),
            pltpu.VMEM((n_slab // 2,) + slot, F32),
            slabs,
            chunked,
            chunked,
            chunked,
            chunked,
            dma,
            dma((2,)),
            dma((n_orb - 1,)),
            dma((n_orb - 1,)),
            dma((n_slab,)),
            dma((n_slab,)),
            dma((3, 2, CHUNKS)),
            dma((3, 2, CHUNKS)),
            dma((n_slab,)),
            dma((n_slab,)),
            dma((n_slab,)),
            dma((n_slab,)),
        ],
        compiler_params=pltpu.CompilerParams(collective_id=0, has_side_effects=True, vmem_limit_bytes=EXCHANGE_VMEM),
        name="exchange",
    )(own, rows)
    action = pl.pallas_call(
        functools.partial(add_kernel, n_pairs, n_orb, orb_dev),
        out_shape=jax.ShapeDtypeStruct(rows.shape, F32),
        in_specs=[SMEM, VMEM, VMEM],
        out_specs=VMEM,
        scratch_shapes=[pltpu.SMEM((2 * n_pairs + TOGETHER,), I32)],
        compiler_params=pltpu.CompilerParams(vmem_limit_bytes=16 << 20),
        name="add",
    )(meta, terms, orb_near)
    action = action.reshape(orb_dev, cells // 128, planes, 128).transpose(0, 2, 1, 3)
    return action.reshape(orb_dev, planes, cells)


def solution(mesh):
    return jax.shard_map(
        body,
        mesh=mesh,
        in_specs=(P("orb", "slab", None), P(("slab", "orb"), None), P(("slab", "orb"), None)),
        out_specs=P("orb", "slab", None),
        check_vma=False,
    )
```

```python
import functools

import jax
import jax.numpy as jnp
import numpy as np
from jax import lax
from jax.experimental import pallas as pl
from jax.experimental.pallas import tpu as pltpu
from jax.sharding import PartitionSpec as P

ITERS = 16
SCREENING = 0.02
CENTER_EIG = 6.0 + SCREENING
HALF_WIDTH = 6.0

MESH = pl.DeviceIdType.MESH
VMEM = pl.BlockSpec(memory_space=pltpu.VMEM)
SMEM = pl.BlockSpec(memory_space=pltpu.SMEM)
F32 = jnp.float32
I32 = jnp.int32
META = 8
CHUNKS = 8
EXCHANGE_VMEM = 50 << 20
UNROLL = 4
TOGETHER = 8


def chebyshev_weights():
    cheb = np.polynomial.chebyshev
    theta, delta = CENTER_EIG, HALF_WIDTH
    sigma = theta / delta
    potential, residue, update = np.zeros(1), np.ones(1), np.ones(1) / theta
    ratio = 1.0 / sigma
    for _ in range(ITERS):
        potential = cheb.chebadd(potential, update)
        applied = cheb.chebsub(theta * update, 6.0 * cheb.chebmulx(update))
        residue = cheb.chebsub(residue, applied)
        ratio_next = 1.0 / (2.0 * sigma - ratio)
        update = cheb.chebadd(ratio_next * ratio * update, 2.0 * ratio_next / delta * residue)
        ratio = ratio_next
    return [float(c) for c in potential[:ITERS]]


WEIGHTS = chebyshev_weights()


SIDE = 4
FAR_FIRST = (2, 1, 3, 0)
STEPS = (0, 2, 1, 3)
NEAR_LAST = (2, 3, 4, 5, 6, 7, 0, 1)


def peers_at(s, dy):
    y, x = s // (2 * SIDE), (s // 2) % SIDE
    row = 2 * SIDE * ((y + dy) % SIDE)
    found = []
    for dx in FAR_FIRST:
        chip = row + 2 * ((x + dx) % SIDE)
        found += [s ^ 1] if dx == dy == 0 else [chip, chip + 1]
    return found


def peers(s):
    return [q for dy in FAR_FIRST for q in peers_at(s, dy)]


def greet(n_slab, n_orb, meanwhile):
    s, o = lax.axis_index("slab"), lax.axis_index("orb")
    barrier = pltpu.get_barrier_semaphore()
    for q in peers(s):
        pl.semaphore_signal(barrier, 1, device_id={"slab": q}, device_id_type=MESH)
    for d in range(1, n_orb):
        pl.semaphore_signal(barrier, 1, device_id={"orb": lax.rem(o + d, n_orb)}, device_id_type=MESH)

    meanwhile()
    pl.semaphore_wait(barrier, n_orb - 1 + n_slab - 1)


def remote(src, dst, send, recv, device):
    return pltpu.make_async_remote_copy(
        src_ref=src, dst_ref=dst, send_sem=send, recv_sem=recv, device_id=device, device_id_type=MESH
    )


def lanes_and_rows():
    lane = lax.broadcasted_iota(I32, (8, 128), 1)
    row = lax.broadcasted_iota(I32, (8, 128), 0)
    return lane, row


def inside_y(j, by, lane, row):
    y = 8 * j + 2 * (row >> 1) + (lane >> 6)
    return ((y - by) & 63) < 32


def split(index, count):
    if count & (count - 1):
        return lax.div(index, count), lax.rem(index, count)
    return index >> (count.bit_length() - 1), index & (count - 1)


def pair_of(meta_ref, p, n_orb):
    slab, at = split(p, n_orb)
    return [meta_ref[slab, 0, META * at + k] for k in range(5)]


def loop(low, high, step):
    def run(n, carry):
        step(n)
        return carry

    lax.fori_loop(low, high, run, 0)


def unrolled(low, high, step):
    def run(n, carry):
        step(n)
        return carry

    lax.fori_loop(low, high, run, 0, unroll=UNROLL)


def share(n_slab, n_orb, own_ref, row, trio, joined, meta_v, send_o, recv_o, send_m, recv_m):
    s, o = lax.axis_index("slab"), lax.axis_index("orb")
    row[...] = jnp.zeros((1, 128), I32)
    row[:, 0:5] = own_ref[...]
    line = pltpu.roll(jnp.broadcast_to(row[...], (8, 128)), META * o, 1)[0:1, :]
    row[...] = line
    trio[o] = line
    copies = [
        remote(row, trio.at[o], send_o.at[d - 1], recv_o.at[d - 1], {"orb": lax.rem(o + d, n_orb)})
        for d in range(1, n_orb)
    ]
    for copy in copies:
        copy.start()
    for copy in copies:
        copy.wait()
    total = trio[0]
    for k in range(1, n_orb):
        total = total + trio[k]
    joined[...] = total
    meta_v[s] = total

    def to(q):
        return remote(joined, meta_v.at[s], send_m.at[q], recv_m.at[s], {"slab": q})

    def arrived(q):
        remote(joined, meta_v.at[q], send_m.at[q], recv_m.at[q], {"slab": q}).wait_recv()

    for q in peers(s):
        to(q).start()
    return arrived, lambda q: to(q).wait_send()


def pack_one(n_orb, orb_dev, meta, orb, packed, dest, q):
    o = lax.axis_index("orb")
    lane, row = lanes_and_rows()
    zz = lane & 63
    i, j, _, by, bz = pair_of(meta, q * n_orb + dest, n_orb)
    (oi, li), (oj, lj) = split(i, orb_dev), split(j, orb_dev)
    hold_i, hold_j = oi == o, oj == o
    whole = []
    for k in range(8):
        a = jnp.where(hold_i, orb[li, 8 * k : 8 * k + 8, :], 1.0)
        b = jnp.where(hold_j, orb[lj, 8 * k : 8 * k + 8, :], 1.0)
        whole.append(a * b)
    folded = []
    for k in range(4):
        v = jnp.where(inside_y(k, by, lane, row), whole[k], whole[k + 4])
        b = bz if k < 2 else (bz + 32) & 63
        folded.append(
            jnp.where(zz + b < 64, pltpu.roll(v, (128 - b) & 127, 1), pltpu.roll(v, (64 - b) & 127, 1))
        )
    for k in range(2):
        packed[dest, q, 8 * k : 8 * k + 8, :] = jnp.where(zz < 32, folded[k], folded[k + 2])


def weight_of(index):
    value = jnp.float32(WEIGHTS[0])
    for k in range(1, ITERS):
        value = jnp.where(index == k, jnp.float32(WEIGHTS[k]), value)
    return value


def cosines(index):
    turn = index & 63
    turn = jnp.minimum(turn, 64 - turn)
    value = jnp.full(index.shape, 1.0, F32)
    for k in range(1, 33):
        value = jnp.where(turn == k, float(np.cos(2.0 * np.pi * k / 64.0)), value)
    return value


def mode_of(m):
    wave = jnp.where(m <= 32, m, m - 32)
    norm = jnp.where((m == 0) | (m == 32), 0.125, 0.125 * float(np.sqrt(2.0)))
    return wave, jnp.where(m <= 32, 0, 16), norm


def modes(to_modes, from_modes, eigen):
    lane, row = lanes_and_rows()
    mode, cell, group = lane & 63, lane & 31, lane >> 5
    wave, quarter, norm = mode_of(mode)
    eigen[...] = (2.0 / 3.0) * cosines(wave)
    zero = jnp.zeros((8, 128), F32)
    for r in range(4):
        table = norm * cosines(wave * (8 * r + row) - quarter)
        for half in range(2):
            part = jnp.where((lane >> 6) == half, table, 0.0)
            for g in range(4):
                top = 128 * half + 32 * g + 8 * r
                for other in range(4):
                    to_modes[top : top + 8, 128 * other : 128 * other + 128] = part if other == g else zero
    for r in range(8):
        wave, quarter, norm = mode_of(8 * r + row)
        table = norm * cosines(wave * cell - quarter)
        for g in range(4):
            part = jnp.where(group == g, table, 0.0)
            for half in range(2):
                top = 128 * g + 64 * half + 8 * r
                for other in range(2):
                    from_modes[top : top + 8, 128 * other : 128 * other + 128] = part if other == half else zero


def exact_dot(a, b):
    return jnp.dot(a, b, precision=lax.Precision.HIGHEST, preferred_element_type=F32)


def solve(bx, by, box, out, rows_a, rows_b, source, ping, pong, to_modes, from_modes, eigen, pairs, wide, halves):
    by32 = by & 31
    lane, row = lanes_and_rows()

    def place(xm):
        x0, x1 = (bx + xm - 8) & 63, (bx + xm + 16) & 63
        at = pl.ds(pl.multiple_of(8 * xm, 8), 8)
        pairs[at, 0:128] = jnp.where(xm >= 8, box[x0 >> 1, pl.ds(x0 & 1, 8, 2), :], 0.0)
        pairs[at, 128:256] = jnp.where(xm < 16, box[x1 >> 1, pl.ds(x1 & 1, 8, 2), :], 0.0)

    unrolled(0, 24, place)
    wide[...] = exact_dot(pairs[...], to_modes[...])

    def spread(xm):
        at = pl.ds(pl.multiple_of(8 * xm, 8), 8)
        for h in range(2):
            for q in range(2):
                g = 2 * h + q
                v = wide[at, 128 * g : 128 * g + 128]
                for dup in range(4):
                    rows_a[xm, pl.ds(32 * dup + 16 * q + h, 8, 2), :] = v

    unrolled(0, 24, spread)

    first = WEIGHTS[ITERS - 1]

    def fill(xm):
        for k in range(6):
            u = 6 * row + k - 8
            v = rows_a[xm, pl.ds(by32 + 24 + k, 8, 6), :]
            v = jnp.where((u >= 0) & (u < 32), v, 0.0)
            source[xm, k] = v
            ping[xm + 1, k] = first * v
            pong[xm + 1, k] = jnp.zeros((8, 128), F32)

    unrolled(0, 24, fill)

    def close(ref):
        for k in range(6):
            ref[0, k] = pltpu.roll(ref[24, k], 64, 1)
            ref[25, k] = pltpu.roll(ref[1, k], 64, 1)

    along_z = eigen[...]

    def doubled(ref, x, at, before, after):
        values = []
        for k in range(6):
            below = at[k - 1] if k > 0 else pltpu.roll(at[5], 1, 0)
            above = at[k + 1] if k < 5 else pltpu.roll(at[0], 7, 0)
            values.append(((before[k] + after[k]) + (below + above)) * (1.0 / 3.0) + along_z * at[k])
        return values

    def sweep(now, finish):
        column = lambda x: [now[x, k] for k in range(6)]
        before, at = column(0), column(1)
        for xm in range(24):
            after = column(xm + 2)
            finish(xm, doubled(now, xm + 1, at, before, after))
            before, at = at, after

    close(ping)

    def step(now, older, index):
        weight = weight_of(index)

        def finish(xm, values):
            for k in range(6):
                older[xm + 1, k] = weight * source[xm, k] + (values[k] - older[xm + 1, k])

        sweep(now, finish)
        close(older)

    def two(n):
        step(ping, pong, ITERS - 2 - 2 * n)
        step(pong, ping, ITERS - 3 - 2 * n)

    loop(0, (ITERS - 2) // 2, two)

    def last(xm, values):
        for k in range(6):
            rows_b[xm, pl.ds(k, 8, 6), :] = WEIGHTS[0] * source[xm, k] + (values[k] * 0.5 - pong[xm + 1, k])

    sweep(ping, last)

    def twice(xm):
        for m in range(4):
            v = rows_b[xm, 8 + 8 * m : 16 + 8 * m, :]
            rows_a[xm, 8 * m : 8 * m + 8, :] = v
            rows_a[xm, 32 + 8 * m : 40 + 8 * m, :] = v

    unrolled(0, 24, twice)

    def collect(xm):
        at = pl.ds(pl.multiple_of(8 * xm, 8), 8)
        for h in range(2):
            for q in range(2):
                g = 2 * h + q
                wide[at, 128 * g : 128 * g + 128] = rows_a[xm, pl.ds(32 - by32 + 16 * q + h, 8, 2), :]

    unrolled(0, 24, collect)
    both = exact_dot(wide[...], from_modes[...])
    for half in range(2):
        halves[:, half] = both[:, 128 * half : 128 * half + 128].reshape(24, 8, 128)

    def give(x2):
        for plane in range(2):
            ux = (2 * x2 + plane - bx) & 31
            half = (ux >= 16).astype(I32)
            xm = ux + 8 - 24 * half
            out[x2, pl.ds(plane, 8, 2), :] = jnp.where(half == 0, halves[xm, 0], halves[xm, 1])

    unrolled(0, 16, give)


def main_kernel(
    n_slab, n_orb, orb_dev, own_ref, orb_hbm, terms, meta_hbm, orb,
    row, trio, joined, meta_v, meta_s, packed, held, relay, combined, density, box,
    rows_a, rows_b, source, ping, pong, to_modes, from_modes, eigen, joint, wide, halves, potential, mine, to_relay, to_plain, to_far, from_dest,
    load_sem, meta_sem, send_o, recv_o, send_m, recv_m, ring_sem, back_sem, send_d, recv_d, send_p, recv_p,
):
    s, o = lax.axis_index("slab"), lax.axis_index("orb")
    half, size = n_slab // 2, n_slab // CHUNKS
    load = pltpu.make_async_copy(orb_hbm, orb, load_sem)
    load.start()
    greet(n_slab, n_orb, lambda: modes(to_modes, from_modes, eigen))
    row_arrived, row_sent = share(
        n_slab, n_orb, own_ref, row, trio, joined, meta_v, send_o, recv_o, send_m, recv_m
    )

    chunks = [
        (2 * ((s // (2 * SIDE) + k) % SIDE) + part, 1 - 2 * part) for k in STEPS for part in range(2)
    ]

    def plane(d):
        return lax.rem(o + d + n_orb, n_orb)

    def rows(c):
        return pl.ds(c * size, size)

    def others(at, act):
        for n in range(size):
            q = chunks[at][0] * size + n
            if at >= 2:
                act(q)
            else:
                pl.when(q != s)(functools.partial(act, q))

    def chunk_loop(c, step):
        unrolled(0, size, lambda n: step(c * size + n, n))

    def ring_copy(kind, sems, source, target, c, d):
        return remote(source, target, sems.at[kind, 0, c], sems.at[kind, 1, c], {"orb": plane(d)})

    def far(c, way):
        return ring_copy(0, ring_sem, packed.at[plane(2), rows(c)], relay.at[c], c, way)

    def through(c, way):
        return ring_copy(1, ring_sem, combined.at[c], held.at[o, rows(c)], c, way)

    def straight(c, way):
        return ring_copy(2, ring_sem, packed.at[plane(-way), rows(c)], held.at[o, rows(c)], c, -way)

    def pack(d, c, into):
        dest = plane(d)
        chunk_loop(c, lambda q, n: pack_one(n_orb, orb_dev, meta_s, orb, into, dest, q))

    def pass_on(c, way):
        far(c, way).wait_recv()

        def step(q, n):
            combined[c, n] = relay[c, n] * packed[plane(way), q]

        chunk_loop(c, step)
        through(c, way).start()

    for at, (c, way) in enumerate(chunks):
        if at % 2 == 0:
            for q in peers_at(s, STEPS[at // 2]):
                row_arrived(q)
            both = pl.ds(c * size, 2 * size)
            local = pltpu.make_async_copy(meta_v.at[both], meta_s.at[both], meta_sem.at[0])
            local.start()
            local.wait()
        if at == 0:
            load.wait()
        pack(2, c, packed)
        far(c, way).start()
    keep = pltpu.make_async_copy(meta_v, meta_hbm, meta_sem.at[1])
    keep.start()
    for at in NEAR_LAST:
        c, way = chunks[at]
        pack(-way, c, packed)
        straight(c, way).start()
    for at in NEAR_LAST:
        c, way = chunks[at]
        pack(way, c, packed)
        pass_on(c, way)
    for c, _ in chunks:
        pack(0, c, held)

    def to_owner(q):
        return remote(density.at[q], box.at[s], send_d.at[q], recv_d.at[s], {"slab": q})

    def from_slab(q):
        return remote(density.at[q], box.at[q], send_d.at[q], recv_d.at[q], {"slab": q})

    for at in NEAR_LAST:
        c, way = chunks[at]
        through(c, way).wait_recv()
        straight(c, way).wait_recv()

        def form(q, n):
            density[q] = held[o, q] * (held[plane(1), q] * held[plane(-1), q])

        chunk_loop(c, form)
        others(at, lambda q: to_owner(q).start())
    box[s] = density[s]
    for q in peers(s):
        from_slab(q).wait_recv()

    _, _, bx, by, _ = pair_of(meta_s, s * n_orb + o, n_orb)
    solve(bx, by, box, potential, rows_a, rows_b, source, ping, pong, to_modes, from_modes, eigen, joint, wide, halves)

    def to_slab(q):
        return remote(potential.at[lax.rem(q, half)], mine.at[s], send_p.at[q], recv_p.at[s], {"slab": q})

    def from_owner(q):
        return remote(potential.at[lax.rem(q, half)], mine.at[q], send_p.at[q], recv_p.at[q], {"slab": q})

    for k in STEPS:
        for q in peers_at(s, k):
            to_slab(q).start()
    mine[s] = potential[lax.rem(s, half)]

    def back_relay(c, way):
        return ring_copy(0, back_sem, to_relay.at[c], from_dest.at[c], c, -way)

    def back_straight(c, way):
        return ring_copy(1, back_sem, to_plain.at[c], terms.at[o, rows(c)], c, way)

    def back_far(c, way):
        return ring_copy(2, back_sem, to_far.at[c], terms.at[plane(way), rows(c)], c, -way)

    def finish(c, way):
        back_relay(c, way).wait_recv()

        def step(q, n):
            value = from_dest[c, n]
            to_far[c, n] = value * packed[plane(way), q]
            terms[plane(way), q] = value * relay[c, n]

        chunk_loop(c, step)
        back_far(c, way).start()

    for at, (c, way) in enumerate(chunks):
        others(at, lambda q: from_owner(q).wait_recv())

        def share_out(q, n):
            own = mine[q] * held[o, q]
            to_relay[c, n] = own * held[plane(way), q]
            to_plain[c, n] = own * held[plane(-way), q]

        chunk_loop(c, share_out)
        back_relay(c, way).start()
        back_straight(c, way).start()
    for c, way in chunks:
        finish(c, way)
    for c, _ in chunks:

        def own_term(q, n):
            terms[o, q] = mine[q] * (held[plane(1), q] * held[plane(-1), q])

        chunk_loop(c, own_term)
    for c, way in chunks:
        back_straight(c, way).wait_recv()
        back_far(c, way).wait_recv()
    for c, way in chunks:
        for copy in (far, through, straight, back_relay, back_straight, back_far):
            copy(c, way).wait_send()

    for q in peers(s):
        row_sent(q)
        to_owner(q).wait_send()
        to_slab(q).wait_send()
    keep.wait()


def add_kernel(n_pairs, n_orb, orb_dev, meta_ref, terms_ref, orb_ref, out_ref, entries):
    s, o = lax.axis_index("slab"), lax.axis_index("orb")
    lane, row = lanes_and_rows()
    z = lane & 63
    x = 2 * s + (row & 1)
    clear = out_ref.shape[1] * orb_dev // n_pairs

    def collect(p, count):
        i, j = pair_of(meta_ref, p, n_orb)[:2]
        (oi, li), (oj, lj) = split(i, orb_dev), split(j, orb_dev)
        both = (oi == oj).astype(I32) * orb_dev
        entries[count] = ((both + lj) * orb_dev + li) * n_pairs + p
        count = count + (oi == o).astype(I32)
        entries[count] = ((both + li) * orb_dev + lj) * n_pairs + p
        count = count + (oj == o).astype(I32)
        at, part = split(p, n_pairs // orb_dev)
        out_ref[at, pl.ds(pl.multiple_of(part * clear, clear), clear), :] = jnp.zeros((clear, 128), F32)
        return count

    count = lax.fori_loop(0, n_pairs, collect, 0, unroll=UNROLL)
    for k in range(TOGETHER):
        entries[count + k] = 0

    def value_of(index):
        rest, p = split(entries[index], n_pairs)
        rest, at = split(rest, orb_dev)
        both, other = split(rest, orb_dev)
        _, _, bx, by, bz = pair_of(meta_ref, p, n_orb)
        owner_slab, owner_orb = split(p, n_orb)
        in_xz = (((x - bx) & 63) < 32) & (((z - bz) & 63) < 32) & (index < count)
        wide = []
        for k in range(4):
            v = terms_ref[owner_orb, owner_slab, 8 * (k % 2) : 8 * (k % 2) + 8, :]
            b = bz if k < 2 else (bz + 32) & 63
            v = jnp.where(z >= b, pltpu.roll(v, b, 1), pltpu.roll(v, (b + 64) & 127, 1))
            wide.append(jnp.where(in_xz, v, 0.0))
        keep = [inside_y(k, by, lane, row) for k in range(4)]
        values = [jnp.where(keep[k], wide[k], 0.0) for k in range(4)]
        values += [jnp.where(keep[k], 0.0, wide[k]) for k in range(4)]
        factors = [jnp.where(both > 0, orb_ref[other, 8 * k : 8 * k + 8, :], 1.0) for k in range(8)]
        return at, [value * factor for value, factor in zip(values, factors)]

    def several(n):
        for at, values in [value_of(TOGETHER * n + k) for k in range(TOGETHER)]:
            for k in range(8):
                out_ref[at, 8 * k : 8 * k + 8, :] = out_ref[at, 8 * k : 8 * k + 8, :] - values[k]

    loop(0, lax.div(count + TOGETHER - 1, TOGETHER), several)


def body(orbitals, pair_list, box_start):
    n_slab, n_orb = lax.axis_size("slab"), lax.axis_size("orb")
    orb_dev, planes, cells = orbitals.shape
    n_pairs = n_slab * n_orb
    slot = (16, 128)
    slots = (n_orb, n_slab) + slot
    rows = orbitals.reshape(orb_dev, planes, cells // 128, 128).transpose(0, 2, 1, 3)
    rows = rows.reshape(orb_dev, planes * cells // 128, 128)
    dma = pltpu.SemaphoreType.DMA
    hbm = pl.BlockSpec(memory_space=pltpu.HBM)
    all_slots, chunked = pltpu.VMEM(slots, F32), pltpu.VMEM((CHUNKS, n_slab // CHUNKS) + slot, F32)
    slabs = pltpu.VMEM((n_slab,) + slot, F32)
    own = jnp.concatenate([pair_list, box_start], axis=1)
    terms, meta, orb_near = pl.pallas_call(
        functools.partial(main_kernel, n_slab, n_orb, orb_dev),
        out_shape=[
            jax.ShapeDtypeStruct(slots, F32),
            jax.ShapeDtypeStruct((n_slab, 1, 128), I32),
            jax.ShapeDtypeStruct(rows.shape, F32),
        ],
        in_specs=[VMEM, hbm],
        out_specs=[VMEM, hbm, VMEM],
        scratch_shapes=[
            pltpu.VMEM((1, 128), I32),
            pltpu.VMEM((n_orb, 1, 128), I32),
            pltpu.VMEM((1, 128), I32),
            pltpu.VMEM((n_slab, 1, 128), I32),
            pltpu.SMEM((n_slab, 1, 128), I32),
            all_slots,
            all_slots,
            chunked,
            chunked,
            slabs,
            slabs,
            pltpu.VMEM((24, 128, 128), F32),
            pltpu.VMEM((24, 48, 128), F32),
            pltpu.VMEM((24, 6, 8, 128), F32),
            pltpu.VMEM((26, 6, 8, 128), F32),
            pltpu.VMEM((26, 6, 8, 128), F32),
            pltpu.VMEM((256, 512), F32),
            pltpu.VMEM((512, 256), F32),
            pltpu.VMEM((8, 128), F32),
            pltpu.VMEM((192, 256), F32),
            pltpu.VMEM((192, 512), F32),
            pltpu.VMEM((24, 2, 8, 128), F32),
            pltpu.VMEM((n_slab // 2,) + slot, F32),
            slabs,
            chunked,
            chunked,
            chunked,
            chunked,
            dma,
            dma((2,)),
            dma((n_orb - 1,)),
            dma((n_orb - 1,)),
            dma((n_slab,)),
            dma((n_slab,)),
            dma((3, 2, CHUNKS)),
            dma((3, 2, CHUNKS)),
            dma((n_slab,)),
            dma((n_slab,)),
            dma((n_slab,)),
            dma((n_slab,)),
        ],
        compiler_params=pltpu.CompilerParams(collective_id=0, has_side_effects=True, vmem_limit_bytes=EXCHANGE_VMEM),
        name="exchange",
    )(own, rows)
    action = pl.pallas_call(
        functools.partial(add_kernel, n_pairs, n_orb, orb_dev),
        out_shape=jax.ShapeDtypeStruct(rows.shape, F32),
        in_specs=[SMEM, VMEM, VMEM],
        out_specs=VMEM,
        scratch_shapes=[pltpu.SMEM((2 * n_pairs + TOGETHER,), I32)],
        compiler_params=pltpu.CompilerParams(vmem_limit_bytes=16 << 20),
        name="add",
    )(meta, terms, orb_near)
    action = action.reshape(orb_dev, cells // 128, planes, 128).transpose(0, 2, 1, 3)
    return action.reshape(orb_dev, planes, cells)


def solution(mesh):
    return jax.shard_map(
        body,
        mesh=mesh,
        in_specs=(P("orb", "slab", None), P(("slab", "orb"), None), P(("slab", "orb"), None)),
        out_specs=P("orb", "slab", None),
        check_vma=False,
    )
```

```python
import functools

import jax
import jax.numpy as jnp
import numpy as np
from jax import lax
from jax.experimental import pallas as pl
from jax.experimental.pallas import tpu as pltpu
from jax.sharding import PartitionSpec as P

ITERS = 16
SCREENING = 0.02
CENTER_EIG = 6.0 + SCREENING
HALF_WIDTH = 6.0

MESH = pl.DeviceIdType.MESH
VMEM = pl.BlockSpec(memory_space=pltpu.VMEM)
SMEM = pl.BlockSpec(memory_space=pltpu.SMEM)
F32 = jnp.float32
I32 = jnp.int32
META = 8
CHUNKS = 8
EXCHANGE_VMEM = 50 << 20
UNROLL = 4
TOGETHER = 8


def chebyshev_weights():
    cheb = np.polynomial.chebyshev
    theta, delta = CENTER_EIG, HALF_WIDTH
    sigma = theta / delta
    potential, residue, update = np.zeros(1), np.ones(1), np.ones(1) / theta
    ratio = 1.0 / sigma
    for _ in range(ITERS):
        potential = cheb.chebadd(potential, update)
        applied = cheb.chebsub(theta * update, 6.0 * cheb.chebmulx(update))
        residue = cheb.chebsub(residue, applied)
        ratio_next = 1.0 / (2.0 * sigma - ratio)
        update = cheb.chebadd(ratio_next * ratio * update, 2.0 * ratio_next / delta * residue)
        ratio = ratio_next
    return [float(c) for c in potential[:ITERS]]


WEIGHTS = chebyshev_weights()


SIDE = 4
FAR_FIRST = (2, 1, 3, 0)
STEPS = (0, 1, 3, 2)
NEAR_LAST = (2, 3, 4, 5, 6, 7, 0, 1)


def peers_at(s, dy):
    y, x = s // (2 * SIDE), (s // 2) % SIDE
    row = 2 * SIDE * ((y + dy) % SIDE)
    found = []
    for dx in FAR_FIRST:
        chip = row + 2 * ((x + dx) % SIDE)
        found += [s ^ 1] if dx == dy == 0 else [chip, chip + 1]
    return found


def peers(s):
    return [q for dy in FAR_FIRST for q in peers_at(s, dy)]


def greet(n_slab, n_orb, meanwhile):
    s, o = lax.axis_index("slab"), lax.axis_index("orb")
    barrier = pltpu.get_barrier_semaphore()
    for q in peers(s):
        pl.semaphore_signal(barrier, 1, device_id={"slab": q}, device_id_type=MESH)
    for d in range(1, n_orb):
        pl.semaphore_signal(barrier, 1, device_id={"orb": lax.rem(o + d, n_orb)}, device_id_type=MESH)

    meanwhile()
    pl.semaphore_wait(barrier, n_orb - 1 + n_slab - 1)


def remote(src, dst, send, recv, device):
    return pltpu.make_async_remote_copy(
        src_ref=src, dst_ref=dst, send_sem=send, recv_sem=recv, device_id=device, device_id_type=MESH
    )


def lanes_and_rows():
    lane = lax.broadcasted_iota(I32, (8, 128), 1)
    row = lax.broadcasted_iota(I32, (8, 128), 0)
    return lane, row


def inside_y(j, by, lane, row):
    y = 8 * j + 2 * (row >> 1) + (lane >> 6)
    return ((y - by) & 63) < 32


def split(index, count):
    if count & (count - 1):
        return lax.div(index, count), lax.rem(index, count)
    return index >> (count.bit_length() - 1), index & (count - 1)


def pair_of(meta_ref, p, n_orb):
    slab, at = split(p, n_orb)
    return [meta_ref[slab, 0, META * at + k] for k in range(5)]


def loop(low, high, step):
    def run(n, carry):
        step(n)
        return carry

    lax.fori_loop(low, high, run, 0)


def unrolled(low, high, step):
    def run(n, carry):
        step(n)
        return carry

    lax.fori_loop(low, high, run, 0, unroll=UNROLL)


def share(n_slab, n_orb, own_ref, row, trio, joined, meta_v, send_o, recv_o, send_m, recv_m):
    s, o = lax.axis_index("slab"), lax.axis_index("orb")
    row[...] = jnp.zeros((1, 128), I32)
    row[:, 0:5] = own_ref[...]
    line = pltpu.roll(jnp.broadcast_to(row[...], (8, 128)), META * o, 1)[0:1, :]
    row[...] = line
    trio[o] = line
    copies = [
        remote(row, trio.at[o], send_o.at[d - 1], recv_o.at[d - 1], {"orb": lax.rem(o + d, n_orb)})
        for d in range(1, n_orb)
    ]
    for copy in copies:
        copy.start()
    for copy in copies:
        copy.wait()
    total = trio[0]
    for k in range(1, n_orb):
        total = total + trio[k]
    joined[...] = total
    meta_v[s] = total

    def to(q):
        return remote(joined, meta_v.at[s], send_m.at[q], recv_m.at[s], {"slab": q})

    def arrived(q):
        remote(joined, meta_v.at[q], send_m.at[q], recv_m.at[q], {"slab": q}).wait_recv()

    for q in peers(s):
        to(q).start()
    return arrived, lambda q: to(q).wait_send()


def pack_one(n_orb, orb_dev, meta, orb, packed, dest, q):
    o = lax.axis_index("orb")
    lane, row = lanes_and_rows()
    zz = lane & 63
    i, j, _, by, bz = pair_of(meta, q * n_orb + dest, n_orb)
    (oi, li), (oj, lj) = split(i, orb_dev), split(j, orb_dev)
    hold_i, hold_j = oi == o, oj == o
    whole = []
    for k in range(8):
        a = jnp.where(hold_i, orb[li, 8 * k : 8 * k + 8, :], 1.0)
        b = jnp.where(hold_j, orb[lj, 8 * k : 8 * k + 8, :], 1.0)
        whole.append(a * b)
    folded = []
    for k in range(4):
        v = jnp.where(inside_y(k, by, lane, row), whole[k], whole[k + 4])
        b = bz if k < 2 else (bz + 32) & 63
        folded.append(
            jnp.where(zz + b < 64, pltpu.roll(v, (128 - b) & 127, 1), pltpu.roll(v, (64 - b) & 127, 1))
        )
    for k in range(2):
        packed[dest, q, 8 * k : 8 * k + 8, :] = jnp.where(zz < 32, folded[k], folded[k + 2])


def weight_of(index):
    value = jnp.float32(WEIGHTS[0])
    for k in range(1, ITERS):
        value = jnp.where(index == k, jnp.float32(WEIGHTS[k]), value)
    return value


def cosines(index):
    turn = index & 63
    turn = jnp.minimum(turn, 64 - turn)
    value = jnp.full(index.shape, 1.0, F32)
    for k in range(1, 33):
        value = jnp.where(turn == k, float(np.cos(2.0 * np.pi * k / 64.0)), value)
    return value


def mode_of(m):
    wave = jnp.where(m <= 32, m, m - 32)
    norm = jnp.where((m == 0) | (m == 32), 0.125, 0.125 * float(np.sqrt(2.0)))
    return wave, jnp.where(m <= 32, 0, 16), norm


def modes(to_modes, from_modes, eigen):
    lane, row = lanes_and_rows()
    mode, cell, group = lane & 63, lane & 31, lane >> 5
    wave, quarter, norm = mode_of(mode)
    eigen[...] = (2.0 / 3.0) * cosines(wave)
    zero = jnp.zeros((8, 128), F32)
    for r in range(4):
        table = norm * cosines(wave * (8 * r + row) - quarter)
        for half in range(2):
            part = jnp.where((lane >> 6) == half, table, 0.0)
            for g in range(4):
                top = 128 * half + 32 * g + 8 * r
                for other in range(4):
                    to_modes[top : top + 8, 128 * other : 128 * other + 128] = part if other == g else zero
    for r in range(8):
        wave, quarter, norm = mode_of(8 * r + row)
        table = norm * cosines(wave * cell - quarter)
        for g in range(4):
            part = jnp.where(group == g, table, 0.0)
            for half in range(2):
                top = 128 * g + 64 * half + 8 * r
                for other in range(2):
                    from_modes[top : top + 8, 128 * other : 128 * other + 128] = part if other == half else zero


def exact_dot(a, b):
    return jnp.dot(a, b, precision=lax.Precision.HIGHEST, preferred_element_type=F32)


def solve(bx, by, box, out, rows_a, rows_b, source, ping, pong, to_modes, from_modes, eigen, pairs, wide, halves):
    by32 = by & 31
    lane, row = lanes_and_rows()

    def place(xm):
        x0, x1 = (bx + xm - 8) & 63, (bx + xm + 16) & 63
        at = pl.ds(pl.multiple_of(8 * xm, 8), 8)
        pairs[at, 0:128] = jnp.where(xm >= 8, box[x0 >> 1, pl.ds(x0 & 1, 8, 2), :], 0.0)
        pairs[at, 128:256] = jnp.where(xm < 16, box[x1 >> 1, pl.ds(x1 & 1, 8, 2), :], 0.0)

    unrolled(0, 24, place)
    wide[...] = exact_dot(pairs[...], to_modes[...])

    def spread(xm):
        at = pl.ds(pl.multiple_of(8 * xm, 8), 8)
        for h in range(2):
            for q in range(2):
                g = 2 * h + q
                v = wide[at, 128 * g : 128 * g + 128]
                for dup in range(4):
                    rows_a[xm, pl.ds(32 * dup + 16 * q + h, 8, 2), :] = v

    unrolled(0, 24, spread)

    first = WEIGHTS[ITERS - 1]

    def fill(xm):
        for k in range(6):
            u = 6 * row + k - 8
            v = rows_a[xm, pl.ds(by32 + 24 + k, 8, 6), :]
            v = jnp.where((u >= 0) & (u < 32), v, 0.0)
            source[xm, k] = v
            ping[xm + 1, k] = first * v
            pong[xm + 1, k] = jnp.zeros((8, 128), F32)

    unrolled(0, 24, fill)

    def close(ref):
        for k in range(6):
            ref[0, k] = pltpu.roll(ref[24, k], 64, 1)
            ref[25, k] = pltpu.roll(ref[1, k], 64, 1)

    along_z = eigen[...]

    def doubled(ref, x, at, before, after):
        values = []
        for k in range(6):
            below = at[k - 1] if k > 0 else pltpu.roll(at[5], 1, 0)
            above = at[k + 1] if k < 5 else pltpu.roll(at[0], 7, 0)
            values.append(((before[k] + after[k]) + (below + above)) * (1.0 / 3.0) + along_z * at[k])
        return values

    def sweep(now, finish):
        column = lambda x: [now[x, k] for k in range(6)]
        before, at = column(0), column(1)
        for xm in range(24):
            after = column(xm + 2)
            finish(xm, doubled(now, xm + 1, at, before, after))
            before, at = at, after

    close(ping)

    def step(now, older, index):
        weight = weight_of(index)

        def finish(xm, values):
            for k in range(6):
                older[xm + 1, k] = weight * source[xm, k] + (values[k] - older[xm + 1, k])

        sweep(now, finish)
        close(older)

    def two(n):
        step(ping, pong, ITERS - 2 - 2 * n)
        step(pong, ping, ITERS - 3 - 2 * n)

    loop(0, (ITERS - 2) // 2, two)

    def last(xm, values):
        for k in range(6):
            rows_b[xm, pl.ds(k, 8, 6), :] = WEIGHTS[0] * source[xm, k] + (values[k] * 0.5 - pong[xm + 1, k])

    sweep(ping, last)

    def twice(xm):
        for m in range(4):
            v = rows_b[xm, 8 + 8 * m : 16 + 8 * m, :]
            rows_a[xm, 8 * m : 8 * m + 8, :] = v
            rows_a[xm, 32 + 8 * m : 40 + 8 * m, :] = v

    unrolled(0, 24, twice)

    def collect(xm):
        at = pl.ds(pl.multiple_of(8 * xm, 8), 8)
        for h in range(2):
            for q in range(2):
                g = 2 * h + q
                wide[at, 128 * g : 128 * g + 128] = rows_a[xm, pl.ds(32 - by32 + 16 * q + h, 8, 2), :]

    unrolled(0, 24, collect)
    both = exact_dot(wide[...], from_modes[...])
    for half in range(2):
        halves[:, half] = both[:, 128 * half : 128 * half + 128].reshape(24, 8, 128)

    def give(x2):
        for plane in range(2):
            ux = (2 * x2 + plane - bx) & 31
            half = (ux >= 16).astype(I32)
            xm = ux + 8 - 24 * half
            out[x2, pl.ds(plane, 8, 2), :] = jnp.where(half == 0, halves[xm, 0], halves[xm, 1])

    unrolled(0, 16, give)


def main_kernel(
    n_slab, n_orb, orb_dev, own_ref, orb_hbm, terms, meta_hbm, orb,
    row, trio, joined, meta_v, meta_s, packed, held, relay, combined, density, box,
    rows_a, rows_b, source, ping, pong, to_modes, from_modes, eigen, joint, wide, halves, potential, mine, to_relay, to_plain, to_far, from_dest,
    load_sem, meta_sem, send_o, recv_o, send_m, recv_m, ring_sem, back_sem, send_d, recv_d, send_p, recv_p,
):
    s, o = lax.axis_index("slab"), lax.axis_index("orb")
    half, size = n_slab // 2, n_slab // CHUNKS
    load = pltpu.make_async_copy(orb_hbm, orb, load_sem)
    load.start()
    greet(n_slab, n_orb, lambda: modes(to_modes, from_modes, eigen))
    row_arrived, row_sent = share(
        n_slab, n_orb, own_ref, row, trio, joined, meta_v, send_o, recv_o, send_m, recv_m
    )

    chunks = [
        (2 * ((s // (2 * SIDE) + k) % SIDE) + part, 1 - 2 * part) for k in STEPS for part in range(2)
    ]

    def plane(d):
        return lax.rem(o + d + n_orb, n_orb)

    def rows(c):
        return pl.ds(c * size, size)

    def others(at, act):
        for n in range(size):
            q = chunks[at][0] * size + n
            if at >= 2:
                act(q)
            else:
                pl.when(q != s)(functools.partial(act, q))

    def chunk_loop(c, step):
        unrolled(0, size, lambda n: step(c * size + n, n))

    def ring_copy(kind, sems, source, target, c, d):
        return remote(source, target, sems.at[kind, 0, c], sems.at[kind, 1, c], {"orb": plane(d)})

    def far(c, way):
        return ring_copy(0, ring_sem, packed.at[plane(2), rows(c)], relay.at[c], c, way)

    def through(c, way):
        return ring_copy(1, ring_sem, combined.at[c], held.at[o, rows(c)], c, way)

    def straight(c, way):
        return ring_copy(2, ring_sem, packed.at[plane(-way), rows(c)], held.at[o, rows(c)], c, -way)

    def pack(d, c, into):
        dest = plane(d)
        chunk_loop(c, lambda q, n: pack_one(n_orb, orb_dev, meta_s, orb, into, dest, q))

    def pass_on(c, way):
        far(c, way).wait_recv()

        def step(q, n):
            combined[c, n] = relay[c, n] * packed[plane(way), q]

        chunk_loop(c, step)
        through(c, way).start()

    for at, (c, way) in enumerate(chunks):
        if at % 2 == 0:
            for q in peers_at(s, STEPS[at // 2]):
                row_arrived(q)
            both = pl.ds(c * size, 2 * size)
            local = pltpu.make_async_copy(meta_v.at[both], meta_s.at[both], meta_sem.at[0])
            local.start()
            local.wait()
        if at == 0:
            load.wait()
        pack(2, c, packed)
        far(c, way).start()
    keep = pltpu.make_async_copy(meta_v, meta_hbm, meta_sem.at[1])
    keep.start()
    for at in NEAR_LAST:
        c, way = chunks[at]
        pack(-way, c, packed)
        straight(c, way).start()
    for at in NEAR_LAST:
        c, way = chunks[at]
        pack(way, c, packed)
        pass_on(c, way)
    for c, _ in chunks:
        pack(0, c, held)

    def to_owner(q):
        return remote(density.at[q], box.at[s], send_d.at[q], recv_d.at[s], {"slab": q})

    def from_slab(q):
        return remote(density.at[q], box.at[q], send_d.at[q], recv_d.at[q], {"slab": q})

    for at in NEAR_LAST:
        c, way = chunks[at]
        through(c, way).wait_recv()
        straight(c, way).wait_recv()

        def form(q, n):
            density[q] = held[o, q] * (held[plane(1), q] * held[plane(-1), q])

        chunk_loop(c, form)
        others(at, lambda q: to_owner(q).start())
    box[s] = density[s]
    for q in peers(s):
        from_slab(q).wait_recv()

    _, _, bx, by, _ = pair_of(meta_s, s * n_orb + o, n_orb)
    solve(bx, by, box, potential, rows_a, rows_b, source, ping, pong, to_modes, from_modes, eigen, joint, wide, halves)

    def to_slab(q):
        return remote(potential.at[lax.rem(q, half)], mine.at[s], send_p.at[q], recv_p.at[s], {"slab": q})

    def from_owner(q):
        return remote(potential.at[lax.rem(q, half)], mine.at[q], send_p.at[q], recv_p.at[q], {"slab": q})

    for k in STEPS:
        for q in reversed(peers_at(s, k)):
            to_slab(q).start()
    mine[s] = potential[lax.rem(s, half)]

    def back_relay(c, way):
        return ring_copy(0, back_sem, to_relay.at[c], from_dest.at[c], c, -way)

    def back_straight(c, way):
        return ring_copy(1, back_sem, to_plain.at[c], terms.at[o, rows(c)], c, way)

    def back_far(c, way):
        return ring_copy(2, back_sem, to_far.at[c], terms.at[plane(way), rows(c)], c, -way)

    def finish(c, way):
        back_relay(c, way).wait_recv()

        def step(q, n):
            value = from_dest[c, n]
            to_far[c, n] = value * packed[plane(way), q]
            terms[plane(way), q] = value * relay[c, n]

        chunk_loop(c, step)
        back_far(c, way).start()

    for at, (c, way) in enumerate(chunks):
        others(at, lambda q: from_owner(q).wait_recv())

        def share_out(q, n):
            own = mine[q] * held[o, q]
            to_relay[c, n] = own * held[plane(way), q]
            to_plain[c, n] = own * held[plane(-way), q]

        chunk_loop(c, share_out)
        back_relay(c, way).start()
        back_straight(c, way).start()
    for c, way in chunks:
        finish(c, way)
    for c, _ in chunks:

        def own_term(q, n):
            terms[o, q] = mine[q] * (held[plane(1), q] * held[plane(-1), q])

        chunk_loop(c, own_term)
    for c, way in chunks:
        back_straight(c, way).wait_recv()
        back_far(c, way).wait_recv()
    for c, way in chunks:
        for copy in (far, through, straight, back_relay, back_straight, back_far):
            copy(c, way).wait_send()

    for q in peers(s):
        row_sent(q)
        to_owner(q).wait_send()
        to_slab(q).wait_send()
    keep.wait()


def add_kernel(n_pairs, n_orb, orb_dev, meta_ref, terms_ref, orb_ref, out_ref, entries):
    s, o = lax.axis_index("slab"), lax.axis_index("orb")
    lane, row = lanes_and_rows()
    z = lane & 63
    x = 2 * s + (row & 1)
    clear = out_ref.shape[1] * orb_dev // n_pairs

    def collect(p, count):
        i, j = pair_of(meta_ref, p, n_orb)[:2]
        (oi, li), (oj, lj) = split(i, orb_dev), split(j, orb_dev)
        both = (oi == oj).astype(I32) * orb_dev
        entries[count] = ((both + lj) * orb_dev + li) * n_pairs + p
        count = count + (oi == o).astype(I32)
        entries[count] = ((both + li) * orb_dev + lj) * n_pairs + p
        count = count + (oj == o).astype(I32)
        at, part = split(p, n_pairs // orb_dev)
        out_ref[at, pl.ds(pl.multiple_of(part * clear, clear), clear), :] = jnp.zeros((clear, 128), F32)
        return count

    count = lax.fori_loop(0, n_pairs, collect, 0, unroll=UNROLL)
    for k in range(TOGETHER):
        entries[count + k] = 0

    def value_of(index):
        rest, p = split(entries[index], n_pairs)
        rest, at = split(rest, orb_dev)
        both, other = split(rest, orb_dev)
        _, _, bx, by, bz = pair_of(meta_ref, p, n_orb)
        owner_slab, owner_orb = split(p, n_orb)
        in_xz = (((x - bx) & 63) < 32) & (((z - bz) & 63) < 32) & (index < count)
        wide = []
        for k in range(4):
            v = terms_ref[owner_orb, owner_slab, 8 * (k % 2) : 8 * (k % 2) + 8, :]
            b = bz if k < 2 else (bz + 32) & 63
            v = jnp.where(z >= b, pltpu.roll(v, b, 1), pltpu.roll(v, (b + 64) & 127, 1))
            wide.append(jnp.where(in_xz, v, 0.0))
        keep = [inside_y(k, by, lane, row) for k in range(4)]
        values = [jnp.where(keep[k], wide[k], 0.0) for k in range(4)]
        values += [jnp.where(keep[k], 0.0, wide[k]) for k in range(4)]
        factors = [jnp.where(both > 0, orb_ref[other, 8 * k : 8 * k + 8, :], 1.0) for k in range(8)]
        return at, [value * factor for value, factor in zip(values, factors)]

    def several(n):
        for at, values in [value_of(TOGETHER * n + k) for k in range(TOGETHER)]:
            for k in range(8):
                out_ref[at, 8 * k : 8 * k + 8, :] = out_ref[at, 8 * k : 8 * k + 8, :] - values[k]

    loop(0, lax.div(count + TOGETHER - 1, TOGETHER), several)


def body(orbitals, pair_list, box_start):
    n_slab, n_orb = lax.axis_size("slab"), lax.axis_size("orb")
    orb_dev, planes, cells = orbitals.shape
    n_pairs = n_slab * n_orb
    slot = (16, 128)
    slots = (n_orb, n_slab) + slot
    rows = orbitals.reshape(orb_dev, planes, cells // 128, 128).transpose(0, 2, 1, 3)
    rows = rows.reshape(orb_dev, planes * cells // 128, 128)
    dma = pltpu.SemaphoreType.DMA
    hbm = pl.BlockSpec(memory_space=pltpu.HBM)
    all_slots, chunked = pltpu.VMEM(slots, F32), pltpu.VMEM((CHUNKS, n_slab // CHUNKS) + slot, F32)
    slabs = pltpu.VMEM((n_slab,) + slot, F32)
    own = jnp.concatenate([pair_list, box_start], axis=1)
    terms, meta, orb_near = pl.pallas_call(
        functools.partial(main_kernel, n_slab, n_orb, orb_dev),
        out_shape=[
            jax.ShapeDtypeStruct(slots, F32),
            jax.ShapeDtypeStruct((n_slab, 1, 128), I32),
            jax.ShapeDtypeStruct(rows.shape, F32),
        ],
        in_specs=[VMEM, hbm],
        out_specs=[VMEM, hbm, VMEM],
        scratch_shapes=[
            pltpu.VMEM((1, 128), I32),
            pltpu.VMEM((n_orb, 1, 128), I32),
            pltpu.VMEM((1, 128), I32),
            pltpu.VMEM((n_slab, 1, 128), I32),
            pltpu.SMEM((n_slab, 1, 128), I32),
            all_slots,
            all_slots,
            chunked,
            chunked,
            slabs,
            slabs,
            pltpu.VMEM((24, 128, 128), F32),
            pltpu.VMEM((24, 48, 128), F32),
            pltpu.VMEM((24, 6, 8, 128), F32),
            pltpu.VMEM((26, 6, 8, 128), F32),
            pltpu.VMEM((26, 6, 8, 128), F32),
            pltpu.VMEM((256, 512), F32),
            pltpu.VMEM((512, 256), F32),
            pltpu.VMEM((8, 128), F32),
            pltpu.VMEM((192, 256), F32),
            pltpu.VMEM((192, 512), F32),
            pltpu.VMEM((24, 2, 8, 128), F32),
            pltpu.VMEM((n_slab // 2,) + slot, F32),
            slabs,
            chunked,
            chunked,
            chunked,
            chunked,
            dma,
            dma((2,)),
            dma((n_orb - 1,)),
            dma((n_orb - 1,)),
            dma((n_slab,)),
            dma((n_slab,)),
            dma((3, 2, CHUNKS)),
            dma((3, 2, CHUNKS)),
            dma((n_slab,)),
            dma((n_slab,)),
            dma((n_slab,)),
            dma((n_slab,)),
        ],
        compiler_params=pltpu.CompilerParams(collective_id=0, has_side_effects=True, vmem_limit_bytes=EXCHANGE_VMEM),
        name="exchange",
    )(own, rows)
    action = pl.pallas_call(
        functools.partial(add_kernel, n_pairs, n_orb, orb_dev),
        out_shape=jax.ShapeDtypeStruct(rows.shape, F32),
        in_specs=[SMEM, VMEM, VMEM],
        out_specs=VMEM,
        scratch_shapes=[pltpu.SMEM((2 * n_pairs + TOGETHER,), I32)],
        compiler_params=pltpu.CompilerParams(vmem_limit_bytes=16 << 20),
        name="add",
    )(meta, terms, orb_near)
    action = action.reshape(orb_dev, cells // 128, planes, 128).transpose(0, 2, 1, 3)
    return action.reshape(orb_dev, planes, cells)


def solution(mesh):
    return jax.shard_map(
        body,
        mesh=mesh,
        in_specs=(P("orb", "slab", None), P(("slab", "orb"), None), P(("slab", "orb"), None)),
        out_specs=P("orb", "slab", None),
        check_vma=False,
    )
```
